32 devices in a mesh: rep: 4 (over x, y), dp: 8 (over z, core).
Axes of the slice: x: 2, y: 2, z: 4, core: 2. Of those that a mesh axis runs over, the one named last changes fastest.
Arguments:
- g_w_gate: bfloat16 [32, 2, 1024, 4096], P(('rep', 'dp')), parts along dimension 0
- g_w_up: bfloat16 [32, 2, 1024, 4096], P(('rep', 'dp')), parts along dimension 0
- g_w_down: bfloat16 [32, 2, 4096, 1024], P(('rep', 'dp')), parts along dimension 0
- w_gate: bfloat16 [2, 1024, 4096], replicated
- w_up: bfloat16 [2, 1024, 4096], replicated
- w_down: bfloat16 [2, 4096, 1024], replicated
- m_w_gate: float32 [2, 1024, 4096], P(None, 'dp')
- m_w_up: float32 [2, 1024, 4096], P(None, 'dp')
- m_w_down: float32 [2, 4096, 1024], P(None, 'dp')
- v_w_gate: float32 [2, 1024, 4096], P(None, 'dp')
- v_w_up: float32 [2, 1024, 4096], P(None, 'dp')
- v_w_down: float32 [2, 4096, 1024], P(None, 'dp')
Outputs:
- output 1: bfloat16 [8, 1024, 4096], P('rep'), parts along dimension 0
- output 2: bfloat16 [8, 1024, 4096], P('rep'), parts along dimension 0
- output 3: bfloat16 [8, 4096, 1024], P('rep'), parts along dimension 0
- output 4: float32 [8, 1024, 4096], P('rep', 'dp'), parts along dimension 0
- output 5: float32 [8, 1024, 4096], P('rep', 'dp'), parts along dimension 0
- output 6: float32 [8, 4096, 1024], P('rep', 'dp'), parts along dimension 0
- output 7: float32 [8, 1024, 4096], P('rep', 'dp'), parts along dimension 0
- output 8: float32 [8, 1024, 4096], P('rep', 'dp'), parts along dimension 0
- output 9: float32 [8, 4096, 1024], P('rep', 'dp'), parts along dimension 0
There are 4 independent parts. The reference program is written for one: setup_inputs(seed, part) draws one part's arguments, and reference() takes and returns one part's arrays. A program takes and returns all parts, laid end to end along the dimension named above; an argument that names none is the same for every part.
All inputs are finite; a program needn't handle non-finite values.
Results may differ from the reference program's by a relative error of at most 0.022.
Values are sent between devices in bfloat16 or wider.
A program may use at most 2 GiB of HBM per device.

```python
import jax
import jax.numpy as jnp
from jax import lax

DEVICES = 8
D = 1024
FF = 4096
LAYERS = 2
NAMES = ("w_gate", "w_up", "w_down")
SHAPES = {"w_gate": (LAYERS, D, FF), "w_up": (LAYERS, D, FF), "w_down": (LAYERS, FF, D)}


def setup_inputs(seed: int = 0, part: int = 0) -> dict:
    kz, *keys = jax.random.split(jax.random.key(seed), 1 + 5 * len(NAMES))
    loud = 2.0 ** jax.random.uniform(kz, (), jnp.float32, -1.0, 1.0)
    drawn = {}
    for name, key, both in zip(NAMES, keys[:3], keys[3:6], strict=True):
        own = jax.random.normal(jax.random.fold_in(key, part), (DEVICES, *SHAPES[name]), jnp.float32)
        shared = jax.random.normal(jax.random.fold_in(both, part), SHAPES[name], jnp.float32)
        drawn["g_" + name] = (loud * (0.7 * shared / DEVICES + 0.7 * own * DEVICES**-0.5)).astype(jnp.bfloat16)
    for name, key in zip(NAMES, keys[6:9], strict=True):
        drawn[name] = (jax.random.normal(key, SHAPES[name], jnp.float32) * SHAPES[name][1] ** -0.5).astype(jnp.bfloat16)
    for name, key in zip(NAMES, keys[9:12], strict=True):
        drawn["m_" + name] = loud * 0.5 * jax.random.normal(key, SHAPES[name], jnp.float32)
    for name, key in zip(NAMES, keys[12:15], strict=True):
        drawn["v_" + name] = loud * loud * jax.random.uniform(key, SHAPES[name], jnp.float32, 0.5, 1.5)
    return drawn


def adamw(w, m, v, g):
    m = 0.9 * m + 0.1 * g
    v = 0.95 * v + 0.05 * g * g
    step = m * lax.rsqrt(v + 1e-8) + 0.1 * w
    return (w - 0.02 * step).astype(jnp.bfloat16), m, v


def clipped(gradients, sum_of_squares, count):
    factor = jnp.minimum(1.0, 0.5 * lax.rsqrt(sum_of_squares / count + 1e-30))
    return [g * factor for g in gradients]


def reference(g_w_gate, g_w_up, g_w_down, w_gate, w_up, w_down, m_w_gate, m_w_up, m_w_down, v_w_gate, v_w_up, v_w_down):
    def total(terms):
        return lax.scan(lambda so_far, term: (so_far + term.astype(jnp.float32), None), jnp.zeros(terms.shape[1:], jnp.float32), terms)[0]

    gradients = [total(terms).astype(jnp.bfloat16).astype(jnp.float32) for terms in (g_w_gate, g_w_up, g_w_down)]
    gradients = clipped(gradients, sum(jnp.sum(g * g) for g in gradients), sum(g.size for g in gradients))
    new = [
        adamw(w.astype(jnp.float32), m, v, g)
        for w, m, v, g in zip((w_gate, w_up, w_down), (m_w_gate, m_w_up, m_w_down), (v_w_gate, v_w_up, v_w_down), gradients, strict=True)
    ]
    return tuple(one[which] for which in range(3) for one in new)
```

```python
import functools
import math

import jax
import jax.numpy as jnp
from jax import lax
from jax.experimental import pallas as pl
from jax.experimental.pallas import tpu as pltpu
from jax.sharding import PartitionSpec as P

MESH = pl.DeviceIdType.MESH
CR, CC = 128, 1024
PER = 24
N = 2 * PER
S = 4
D = 2
ROWS = 16


def kernel(count, *refs):
    terms, weights, ms, vs = refs[0:3], refs[3:6], refs[6:9], refs[9:12]
    wo, mo, vo = refs[12:15], refs[15:18], refs[18:21]
    (own, par, up, snd, gbuf, acc, nrm, fac, mb, vb, wb, mq, vq,
     own_s, par_s, give_s, up_s, snd_s, par_c, up_c, g_s, gs_s, w_s, out_s, pr_s, ps_s, loc_s, in_s, mv_s, n_s, ns_s) = refs[21:]

    d = lax.axis_index("dp")
    z, c = d // 2, d % 2
    right = z >= 2
    is_end = (z == 0) | (z == 3)
    is_in = (z == 1) | (z == 2)
    mine = jnp.where(right, 2, 1)
    end = jnp.where(right, 3, 0)
    other = 3 - mine
    far = 3 - end
    partner = d + 1 - 2 * c

    def dev(zz):
        return {"dp": 2 * zz + c}

    buddy = {"dp": partner}

    def block_of(s, b):
        return 2 + b if s == 0 else 1 - b

    def by_array(i, fn):
        for a in range(3):
            @pl.when((i >= 8 * a) & (i < 8 * a + 8))
            def _():
                t = i - 8 * a
                fn(a, t // 4, t % 4)

    def whole(ref, a, layer, q, dd, lead=()):
        if a < 2:
            return ref.at[(*lead, layer, pl.ds(pl.multiple_of(dd * 128, 128), CR), pl.ds(pl.multiple_of(q * CC, CC), CC))]
        return ref.at[(*lead, layer, pl.ds(pl.multiple_of(dd * 512 + q * 128, 128), CR), pl.ds(0, CC))]

    def block(ref, a, layer, q):
        if a < 2:
            return ref.at[layer, pl.ds(0, CR), pl.ds(pl.multiple_of(q * CC, CC), CC)]
        return ref.at[layer, pl.ds(pl.multiple_of(q * 128, 128), CR), pl.ds(0, CC)]

    def wait(ref, sem):
        pltpu.make_async_copy(ref, ref, sem).wait()

    def remote(src, dst, ssem, rsem, to):
        return pltpu.make_async_remote_copy(src, dst, ssem, rsem, device_id=to, device_id_type=MESH)

    def start_own(s, j):
        slot = lax.rem(j, S)
        dd = 2 * block_of(s, j // PER) + c

        def go(a, layer, q):
            pltpu.make_async_copy(whole(terms[a], a, layer, q, dd, (0,)), own.at[s, slot], own_s.at[s, slot]).start()

        by_array(lax.rem(j, PER), go)

    def start_give(s, j):
        slot = lax.rem(j, S)
        dd = 2 * block_of(s, j // PER) + 1 - c

        def go(a, layer, q):
            remote(whole(terms[a], a, layer, q, dd, (0,)), par.at[s, slot], give_s.at[s, slot], par_s.at[s, slot], buddy).start()

        by_array(lax.rem(j, PER), go)

    for s in range(2):
        for j in range(S):
            start_own(s, jnp.int32(j))

    barrier = pltpu.get_barrier_semaphore()
    for k in range(1, 8):
        pl.semaphore_signal(barrier, inc=1, device_id={"dp": lax.rem(d + k, 8)}, device_id_type=MESH)
    pl.semaphore_wait(barrier, 7)

    for s in range(2):
        for j in range(S):
            start_give(s, jnp.int32(j))

    acc[...] = jnp.zeros_like(acc)

    def rows(fn):
        def go(r, carry):
            fn(pl.ds(pl.multiple_of(r * ROWS, ROWS), ROWS))
            return carry

        lax.fori_loop(0, CR // ROWS, go, 0)

    def f32(x):
        return x.astype(jnp.float32)

    def process(s, k):
        zz = z if s == 0 else 3 - z
        down = z + 1 if s == 0 else z - 1
        above = z - 1 if s == 0 else z + 1
        j = k - D * zz

        @pl.when((j >= 0) & (j < N))
        def _():
            slot = lax.rem(j, S)
            wait(own.at[s, slot], own_s.at[s, slot])
            wait(par.at[s, slot], par_s.at[s, slot])

            @pl.when((zz < 3) & (j >= S))
            def _():
                wait(snd.at[s, slot], snd_s.at[s, slot])

            @pl.when(zz == 0)
            def _():
                def add(r):
                    snd[s, slot, r, :] = (f32(own[s, slot, r, :]) + f32(par[s, slot, r, :])).astype(jnp.bfloat16)

                rows(add)

            @pl.when(zz > 0)
            def _():
                wait(up.at[s, slot], up_s.at[s, slot])

            @pl.when((zz > 0) & (zz < 3))
            def _():
                def add(r):
                    snd[s, slot, r, :] = (f32(up[s, slot, r, :]) + (f32(own[s, slot, r, :]) + f32(par[s, slot, r, :]))).astype(jnp.bfloat16)

                rows(add)

            @pl.when(zz == 3)
            def _():
                def add(r):
                    g = (f32(up[s, slot, r, :]) + (f32(own[s, slot, r, :]) + f32(par[s, slot, r, :]))).astype(jnp.bfloat16)
                    gbuf[j, r, :] = g
                    acc[...] += f32(g) * f32(g)

                rows(add)

            @pl.when(j < N - S)
            def _():
                pl.semaphore_signal(par_c.at[s], inc=1, device_id=buddy, device_id_type=MESH)

            @pl.when((zz > 0) & (j < N - S))
            def _():
                pl.semaphore_signal(up_c.at[s], inc=1, device_id=dev(above), device_id_type=MESH)

            @pl.when(j + S < N)
            def _():
                start_own(s, j + S)

            @pl.when(zz < 3)
            def _():
                @pl.when(j >= S)
                def _():
                    pl.semaphore_wait(up_c.at[s], 1)

                remote(snd.at[s, slot], up.at[s, slot], snd_s.at[s, slot], up_s.at[s, slot], dev(down)).start()

            @pl.when((j >= 1) & (j + S - 1 < N))
            def _():
                again = lax.rem(j + S - 1, S)
                pl.semaphore_wait(par_c.at[s], 1)
                wait(par.at[s, again], give_s.at[s, again])
                start_give(s, j + S - 1)

    def send_sums():
        def go(i, carry):
            remote(gbuf.at[i], gbuf.at[i], gs_s, g_s.at[i], dev(mine)).start()
            return carry

        lax.fori_loop(0, PER, go, 0)

    def step(k, carry):
        process(0, k)
        process(1, k)

        @pl.when(is_end & (k == N))
        def _():
            send_sums()

        return carry

    lax.fori_loop(0, N + 3 * D, step, 0)

    def start_mvw(i):
        slot = lax.rem(i, 2)

        def go(a, layer, q):
            pltpu.make_async_copy(block(ms[a], a, layer, q), mb.at[slot], in_s.at[slot, 0]).start()
            pltpu.make_async_copy(block(vs[a], a, layer, q), vb.at[slot], in_s.at[slot, 1]).start()
            pltpu.make_async_copy(whole(weights[a], a, layer, q, d), wb.at[slot], in_s.at[slot, 2]).start()

        by_array(i, go)

    start_mvw(jnp.int32(0))

    slot_of = jnp.where(right, 2, 0) + c

    @pl.when(is_end)
    def _():
        part = acc[0:8, 0:128]
        for r in range(ROWS // 8):
            for q in range(CC // 128):
                if r + q:
                    part = part + acc[8 * r : 8 * r + 8, 128 * q : 128 * q + 128]
        nrm[slot_of] = part
        for k in range(1, 8):
            remote(nrm.at[slot_of], nrm.at[slot_of], ns_s.at[k], n_s.at[slot_of], {"dp": lax.rem(d + k, 8)}).start()

    for s in range(2):
        for q in range(S):
            wait(par.at[s, q], give_s.at[s, q])
        zz = z if s == 0 else 3 - z

        @pl.when(zz < 3)
        def _():
            for q in range(S):
                wait(snd.at[s, q], snd_s.at[s, q])

    for k in range(4):
        @pl.when(jnp.logical_not(is_end & (slot_of == k)))
        def _():
            wait(nrm.at[k], n_s.at[k])

    total = jnp.sum((nrm[0] + nrm[1]) + (nrm[2] + nrm[3]), keepdims=True)
    fac[...] = jnp.broadcast_to(jnp.minimum(1.0, 0.5 * lax.rsqrt(total / count + 1e-30)), fac.shape)

    base = jnp.where(is_end, PER, 0)

    def update(i, carry):
        slot = lax.rem(i, 2)
        at = base + i

        @pl.when(i + 1 < PER)
        def _():
            start_mvw(i + 1)

        wait(mb.at[slot], in_s.at[slot, 0])
        wait(vb.at[slot], in_s.at[slot, 1])
        wait(wb.at[slot], in_s.at[slot, 2])

        @pl.when(i >= 2)
        def _():
            wait(mq.at[slot], mv_s.at[slot, 0])
            wait(vq.at[slot], mv_s.at[slot, 1])

        @pl.when(is_in)
        def _():
            wait(gbuf.at[i], g_s.at[i])

        def adam(r):
            g = f32(gbuf[at, r, :]) * fac[...]
            m = 0.9 * mb[slot, r, :] + 0.1 * g
            v = 0.95 * vb[slot, r, :] + 0.05 * g * g
            w = f32(wb[slot, r, :])
            mq[slot, r, :] = m
            vq[slot, r, :] = v
            gbuf[at, r, :] = (w - 0.02 * (m * lax.rsqrt(v + 1e-8) + 0.1 * w)).astype(jnp.bfloat16)

        rows(adam)

        def go(a, layer, q):
            new = gbuf.at[at]
            there = whole(wo[a], a, layer, q, d)
            pltpu.make_async_copy(mq.at[slot], block(mo[a], a, layer, q), mv_s.at[slot, 0]).start()
            pltpu.make_async_copy(vq.at[slot], block(vo[a], a, layer, q), mv_s.at[slot, 1]).start()

            @pl.when(is_end)
            def _():
                remote(new, there, out_s.at[0], w_s.at[z, i], dev(mine)).start()

            @pl.when(is_in)
            def _():
                remote(new, there, out_s.at[0], w_s.at[z, i], dev(end)).start()
                remote(new, there, out_s.at[1], w_s.at[z, i], dev(other)).start()

            remote(new, there, ps_s.at[z], pr_s.at[z], buddy).start()
            pltpu.make_async_copy(new, there, loc_s).start()

        by_array(i, go)
        return carry

    lax.fori_loop(0, PER, update, 0)

    def pass_on(i, src, over):
        def go(a, layer, q):
            here = whole(wo[a], a, layer, q, 2 * src + c)
            wait(here, w_s.at[src, i])
            if over is not None:
                remote(here, here, out_s.at[over[0]], w_s.at[src, i], dev(over[1])).start()
            remote(here, here, ps_s.at[src], pr_s.at[src], buddy).start()

        by_array(i, go)

    @pl.when(is_in)
    def _():
        def one(i, carry):
            pass_on(i, other, (3, end))
            pass_on(i, end, (2, other))
            return carry

        lax.fori_loop(0, PER, one, 0)

        def two(i, carry):
            pass_on(i, far, (4, end))
            return carry

        lax.fori_loop(0, PER, two, 0)

    @pl.when(is_end)
    def _():
        for src in (mine, other, far):
            def one(i, carry):
                pass_on(i, src, None)
                return carry

            lax.fori_loop(0, PER, one, 0)

    for slot in range(2):
        wait(mq.at[slot], mv_s.at[slot, 0])
        wait(vq.at[slot], mv_s.at[slot, 1])
    six = gbuf.at[pl.ds(0, PER)]
    wait(six, loc_s)
    wait(six, out_s.at[0])

    @pl.when(is_in)
    def _():
        for k in range(1, 5):
            wait(six, out_s.at[k])

    @pl.when(is_end)
    def _():
        wait(six, gs_s)
        for k in range(1, 8):
            wait(nrm.at[slot_of], ns_s.at[k])

    for k in range(4):
        wait(six, ps_s.at[k])
        wait(six, pr_s.at[k])


def solution(mesh):
    def step(*arrays):
        weights, m = arrays[3:6], arrays[6:9]
        count = float(8 * sum(math.prod(a.shape) for a in m))
        any_ = pl.BlockSpec(memory_space=pl.ANY)
        chunk = (CR, CC)
        dma, regular = pltpu.SemaphoreType.DMA, pltpu.SemaphoreType.REGULAR
        out = [jax.ShapeDtypeStruct(w.shape, jnp.bfloat16) for w in weights] + [jax.ShapeDtypeStruct(a.shape, jnp.float32) for a in m] * 2
        return pl.pallas_call(
            functools.partial(kernel, count),
            out_shape=out,
            in_specs=[any_] * 12,
            out_specs=[any_] * 9,
            scratch_shapes=[
                pltpu.VMEM((2, S, *chunk), jnp.bfloat16),
                pltpu.VMEM((2, S, *chunk), jnp.bfloat16),
                pltpu.VMEM((2, S, *chunk), jnp.bfloat16),
                pltpu.VMEM((2, S, *chunk), jnp.bfloat16),
                pltpu.VMEM((N, *chunk), jnp.bfloat16),
                pltpu.VMEM((ROWS, CC), jnp.float32),
                pltpu.VMEM((4, 8, 128), jnp.float32),
                pltpu.VMEM((1, CC), jnp.float32),
                pltpu.VMEM((2, *chunk), jnp.float32),
                pltpu.VMEM((2, *chunk), jnp.float32),
                pltpu.VMEM((2, *chunk), jnp.bfloat16),
                pltpu.VMEM((2, *chunk), jnp.float32),
                pltpu.VMEM((2, *chunk), jnp.float32),
                dma((2, S)),
                dma((2, S)),
                dma((2, S)),
                dma((2, S)),
                dma((2, S)),
                regular((2,)),
                regular((2,)),
                dma((PER,)),
                dma,
                dma((4, PER)),
                dma((5,)),
                dma((4,)),
                dma((4,)),
                dma,
                dma((2, 3)),
                dma((2, 2)),
                dma((4,)),
                dma((8,)),
            ],
            compiler_params=pltpu.CompilerParams(collective_id=0, has_side_effects=True, vmem_limit_bytes=40 * 2**20),
            cost_estimate=pl.CostEstimate(flops=10**9, bytes_accessed=3 * 10**8, transcendentals=3 * 2**20),
        )(*arrays)

    all_of, cut = P(None, None, None), P(None, "dp", None)
    return jax.shard_map(
        step,
        mesh=mesh,
        in_specs=(P(("rep", "dp"), None, None, None),) * 3 + (all_of,) * 3 + (cut,) * 6,
        out_specs=(P("rep", None, None),) * 3 + (P("rep", "dp", None),) * 6,
        check_vma=False,
    )
```

```python
import functools
import math

import jax
import jax.numpy as jnp
from jax import lax
from jax.experimental import pallas as pl
from jax.experimental.pallas import tpu as pltpu
from jax.sharding import PartitionSpec as P

MESH = pl.DeviceIdType.MESH
CR, CC = 128, 1024
PER = 24
N = 2 * PER
S = 4
D = 2
W = 3
AHEAD = 3 * D
LAG = 3
ROWS = 16


def kernel(count, *refs):
    terms, weights, ms, vs = refs[0:3], refs[3:6], refs[6:9], refs[9:12]
    wo, mo, vo = refs[12:15], refs[15:18], refs[18:21]
    (own, par, up, snd, gbuf, acc, nrm, fac, mb, vb, wb, mq, vq,
     own_s, par_s, give_s, up_s, snd_s, par_c, up_c, g_s, w_s, out_s, pr_s, ps_s, loc_s, in_s, mv_s, n_s, ns_s) = refs[21:]

    d = lax.axis_index("dp")
    z, c = d // 2, d % 2
    right = z >= 2
    is_end = (z == 0) | (z == 3)
    is_in = (z == 1) | (z == 2)
    mine = jnp.where(right, 2, 1)
    end = jnp.where(right, 3, 0)
    other = 3 - mine
    far = 3 - end
    partner = d + 1 - 2 * c

    def dev(zz):
        return {"dp": 2 * zz + c}

    buddy = {"dp": partner}

    def block_of(s, b):
        return 2 + b if s == 0 else 1 - b

    def by_array(i, fn):
        for a in range(3):
            @pl.when((i >= 8 * a) & (i < 8 * a + 8))
            def _():
                t = i - 8 * a
                fn(a, t // 4, t % 4)

    def whole(ref, a, layer, q, dd, lead=()):
        if a < 2:
            return ref.at[(*lead, layer, pl.ds(pl.multiple_of(dd * 128, 128), CR), pl.ds(pl.multiple_of(q * CC, CC), CC))]
        return ref.at[(*lead, layer, pl.ds(pl.multiple_of(dd * 512 + q * 128, 128), CR), pl.ds(0, CC))]

    def block(ref, a, layer, q):
        if a < 2:
            return ref.at[layer, pl.ds(0, CR), pl.ds(pl.multiple_of(q * CC, CC), CC)]
        return ref.at[layer, pl.ds(pl.multiple_of(q * 128, 128), CR), pl.ds(0, CC)]

    def wait(ref, sem):
        pltpu.make_async_copy(ref, ref, sem).wait()

    def remote(src, dst, ssem, rsem, to):
        return pltpu.make_async_remote_copy(src, dst, ssem, rsem, device_id=to, device_id_type=MESH)

    def start_own(s, j):
        slot = lax.rem(j, S)
        dd = 2 * block_of(s, j // PER) + c

        def go(a, layer, q):
            pltpu.make_async_copy(whole(terms[a], a, layer, q, dd, (0,)), own.at[s, slot], own_s.at[s, slot]).start()

        by_array(lax.rem(j, PER), go)

    def start_give(s, j):
        slot = lax.rem(j, S)
        dd = 2 * block_of(s, j // PER) + 1 - c

        def go(a, layer, q):
            remote(whole(terms[a], a, layer, q, dd, (0,)), par.at[s, slot], give_s.at[s, slot], par_s.at[s, slot], buddy).start()

        by_array(lax.rem(j, PER), go)

    for s in range(2):
        for j in range(S):
            start_own(s, jnp.int32(j))

    barrier = pltpu.get_barrier_semaphore()
    for k in range(1, 8):
        pl.semaphore_signal(barrier, inc=1, device_id={"dp": lax.rem(d + k, 8)}, device_id_type=MESH)
    pl.semaphore_wait(barrier, 7)

    for s in range(2):
        for j in range(S):
            start_give(s, jnp.int32(j))

    acc[...] = jnp.zeros_like(acc)

    def rows(fn):
        def go(r, carry):
            fn(pl.ds(pl.multiple_of(r * ROWS, ROWS), ROWS))
            return carry

        lax.fori_loop(0, CR // ROWS, go, 0)

    def f32(x):
        return x.astype(jnp.float32)

    def process(s, k):
        zz = z if s == 0 else 3 - z
        down = z + 1 if s == 0 else z - 1
        above = z - 1 if s == 0 else z + 1
        j = k - D * zz

        @pl.when((j >= 0) & (j < N))
        def _():
            slot = lax.rem(j, S)
            wait(own.at[s, slot], own_s.at[s, slot])
            wait(par.at[s, slot], par_s.at[s, slot])

            @pl.when((zz < 3) & (j >= S))
            def _():
                wait(snd.at[s, slot], snd_s.at[s, slot])

            @pl.when(zz == 0)
            def _():
                def add(r):
                    snd[s, slot, r, :] = (f32(own[s, slot, r, :]) + f32(par[s, slot, r, :])).astype(jnp.bfloat16)

                rows(add)

            @pl.when(zz > 0)
            def _():
                wait(up.at[s, slot], up_s.at[s, slot])

            @pl.when((zz > 0) & (zz < 3))
            def _():
                def add(r):
                    snd[s, slot, r, :] = (f32(up[s, slot, r, :]) + (f32(own[s, slot, r, :]) + f32(par[s, slot, r, :]))).astype(jnp.bfloat16)

                rows(add)

            @pl.when(zz == 3)
            def _():
                def add(r):
                    g = (f32(up[s, slot, r, :]) + (f32(own[s, slot, r, :]) + f32(par[s, slot, r, :]))).astype(jnp.bfloat16)
                    gbuf[j, r, :] = g
                    acc[...] += f32(g) * f32(g)

                rows(add)

            @pl.when(j < N - S)
            def _():
                pl.semaphore_signal(par_c.at[s], inc=1, device_id=buddy, device_id_type=MESH)

            @pl.when((zz > 0) & (j < N - S))
            def _():
                pl.semaphore_signal(up_c.at[s], inc=1, device_id=dev(above), device_id_type=MESH)

            @pl.when(j + S < N)
            def _():
                start_own(s, j + S)

            @pl.when(zz < 3)
            def _():
                @pl.when(j >= S)
                def _():
                    pl.semaphore_wait(up_c.at[s], 1)

                remote(snd.at[s, slot], up.at[s, slot], snd_s.at[s, slot], up_s.at[s, slot], dev(down)).start()

            @pl.when((j >= 1) & (j + S - 1 < N))
            def _():
                again = lax.rem(j + S - 1, S)
                pl.semaphore_wait(par_c.at[s], 1)
                wait(par.at[s, again], give_s.at[s, again])
                start_give(s, j + S - 1)

    def room(link, u):
        @pl.when(u >= W)
        def _():
            wait(gbuf.at[0], out_s.at[link, lax.rem(u, W)])

    def send_sum(u):
        room(0, u)
        remote(gbuf.at[u], gbuf.at[u], out_s.at[0, lax.rem(u, W)], g_s.at[u], dev(mine)).start()

    def step(k, carry):
        process(0, k)
        process(1, k)

        @pl.when(is_end & (k >= N))
        def _():
            send_sum(k - N)

        return carry

    lax.fori_loop(0, N + 3 * D, step, 0)

    def start_mvw(i):
        slot = lax.rem(i, 2)

        def go(a, layer, q):
            pltpu.make_async_copy(block(ms[a], a, layer, q), mb.at[slot], in_s.at[slot, 0]).start()
            pltpu.make_async_copy(block(vs[a], a, layer, q), vb.at[slot], in_s.at[slot, 1]).start()
            pltpu.make_async_copy(whole(weights[a], a, layer, q, d), wb.at[slot], in_s.at[slot, 2]).start()

        by_array(i, go)

    start_mvw(jnp.int32(0))

    slot_of = jnp.where(right, 2, 0) + c

    @pl.when(is_end)
    def _():
        part = acc[0:8, 0:128]
        for r in range(ROWS // 8):
            for q in range(CC // 128):
                if r + q:
                    part = part + acc[8 * r : 8 * r + 8, 128 * q : 128 * q + 128]
        nrm[slot_of] = part
        for k in range(1, 8):
            remote(nrm.at[slot_of], nrm.at[slot_of], ns_s.at[k], n_s.at[slot_of], {"dp": lax.rem(d + k, 8)}).start()

    for s in range(2):
        for q in range(S):
            wait(par.at[s, q], give_s.at[s, q])
        zz = z if s == 0 else 3 - z

        @pl.when(zz < 3)
        def _():
            for q in range(S):
                wait(snd.at[s, q], snd_s.at[s, q])

    for k in range(4):
        @pl.when(jnp.logical_not(is_end & (slot_of == k)))
        def _():
            wait(nrm.at[k], n_s.at[k])

    total = jnp.sum((nrm[0] + nrm[1]) + (nrm[2] + nrm[3]), keepdims=True)
    fac[...] = jnp.broadcast_to(jnp.minimum(1.0, 0.5 * lax.rsqrt(total / count + 1e-30)), fac.shape)

    base = jnp.where(is_end, PER, 0)

    def update(i):
        slot = lax.rem(i, 2)
        at = base + i

        @pl.when(i + 1 < PER)
        def _():
            start_mvw(i + 1)

        wait(mb.at[slot], in_s.at[slot, 0])
        wait(vb.at[slot], in_s.at[slot, 1])
        wait(wb.at[slot], in_s.at[slot, 2])

        @pl.when(i >= 2)
        def _():
            wait(mq.at[slot], mv_s.at[slot, 0])
            wait(vq.at[slot], mv_s.at[slot, 1])

        @pl.when(is_in)
        def _():
            wait(gbuf.at[i], g_s.at[i])

        def adam(r):
            g = f32(gbuf[at, r, :]) * fac[...]
            m = 0.9 * mb[slot, r, :] + 0.1 * g
            v = 0.95 * vb[slot, r, :] + 0.05 * g * g
            w = f32(wb[slot, r, :])
            mq[slot, r, :] = m
            vq[slot, r, :] = v
            gbuf[at, r, :] = (w - 0.02 * (m * lax.rsqrt(v + 1e-8) + 0.1 * w)).astype(jnp.bfloat16)

        rows(adam)

        @pl.when(is_in)
        def _():
            room(0, i)
            room(1, i)

        def go(a, layer, q):
            new = gbuf.at[at]
            there = whole(wo[a], a, layer, q, d)
            pltpu.make_async_copy(mq.at[slot], block(mo[a], a, layer, q), mv_s.at[slot, 0]).start()
            pltpu.make_async_copy(vq.at[slot], block(vo[a], a, layer, q), mv_s.at[slot, 1]).start()

            @pl.when(is_in)
            def _():
                remote(new, there, out_s.at[0, lax.rem(i, W)], w_s.at[z, i], dev(end)).start()
                remote(new, there, out_s.at[1, lax.rem(i, W)], w_s.at[z, i], dev(other)).start()

            remote(new, there, ps_s.at[z], pr_s.at[z], buddy).start()
            pltpu.make_async_copy(new, there, loc_s).start()

        by_array(i, go)

    def send_new(i, u):
        room(0, u)

        def go(a, layer, q):
            remote(gbuf.at[PER + i], whole(wo[a], a, layer, q, d), out_s.at[0, lax.rem(u, W)], w_s.at[z, i], dev(mine)).start()

        by_array(i, go)

    def pass_on(i, src, over):
        if over is not None:
            room(over[0], over[1])

        def go(a, layer, q):
            here = whole(wo[a], a, layer, q, 2 * src + c)
            wait(here, w_s.at[src, i])
            if over is not None:
                remote(here, here, out_s.at[over[0], lax.rem(over[1], W)], w_s.at[src, i], dev(over[2])).start()
            remote(here, here, ps_s.at[src], pr_s.at[src], buddy).start()

        by_array(i, go)

    @pl.when(is_in)
    def _():
        def first(t, carry):
            update(t)
            return carry

        lax.fori_loop(0, PER, first, 0)

        def second(i, carry):
            pass_on(i, other, (0, PER + i, end))
            pass_on(i, end, (1, PER + i, other))
            return carry

        lax.fori_loop(0, PER, second, 0)

        def third(i, carry):
            pass_on(i, far, (0, 2 * PER + i, end))
            return carry

        lax.fori_loop(0, PER, third, 0)

    @pl.when(is_end)
    def _():
        def tick(t, carry):
            u = t + AHEAD

            @pl.when(u < PER)
            def _():
                send_sum(u)

            @pl.when(t < PER)
            def _():
                update(t)

            @pl.when((u >= PER) & (u < 2 * PER))
            def _():
                send_new(u - PER, u)

            got = t - LAG

            @pl.when((got >= 0) & (got < 3 * PER))
            def _():
                which = got // PER
                pass_on(lax.rem(got, PER), jnp.where(which == 0, mine, jnp.where(which == 1, other, far)), None)

            return carry

        lax.fori_loop(0, 3 * PER + LAG, tick, 0)

    for slot in range(2):
        wait(mq.at[slot], mv_s.at[slot, 0])
        wait(vq.at[slot], mv_s.at[slot, 1])
    six = gbuf.at[pl.ds(0, PER)]
    wait(six, loc_s)
    for k in range(W):
        wait(gbuf.at[0], out_s.at[0, k])

    @pl.when(is_in)
    def _():
        for k in range(W):
            wait(gbuf.at[0], out_s.at[1, k])

    @pl.when(is_end)
    def _():
        for k in range(1, 8):
            wait(nrm.at[slot_of], ns_s.at[k])

    for k in range(4):
        wait(six, ps_s.at[k])
        wait(six, pr_s.at[k])


def solution(mesh):
    def step(*arrays):
        weights, m = arrays[3:6], arrays[6:9]
        count = float(8 * sum(math.prod(a.shape) for a in m))
        any_ = pl.BlockSpec(memory_space=pl.ANY)
        chunk = (CR, CC)
        dma, regular = pltpu.SemaphoreType.DMA, pltpu.SemaphoreType.REGULAR
        out = [jax.ShapeDtypeStruct(w.shape, jnp.bfloat16) for w in weights] + [jax.ShapeDtypeStruct(a.shape, jnp.float32) for a in m] * 2
        return pl.pallas_call(
            functools.partial(kernel, count),
            out_shape=out,
            in_specs=[any_] * 12,
            out_specs=[any_] * 9,
            scratch_shapes=[
                pltpu.VMEM((2, S, *chunk), jnp.bfloat16),
                pltpu.VMEM((2, S, *chunk), jnp.bfloat16),
                pltpu.VMEM((2, S, *chunk), jnp.bfloat16),
                pltpu.VMEM((2, S, *chunk), jnp.bfloat16),
                pltpu.VMEM((N, *chunk), jnp.bfloat16),
                pltpu.VMEM((ROWS, CC), jnp.float32),
                pltpu.VMEM((4, 8, 128), jnp.float32),
                pltpu.VMEM((1, CC), jnp.float32),
                pltpu.VMEM((2, *chunk), jnp.float32),
                pltpu.VMEM((2, *chunk), jnp.float32),
                pltpu.VMEM((2, *chunk), jnp.bfloat16),
                pltpu.VMEM((2, *chunk), jnp.float32),
                pltpu.VMEM((2, *chunk), jnp.float32),
                dma((2, S)),
                dma((2, S)),
                dma((2, S)),
                dma((2, S)),
                dma((2, S)),
                regular((2,)),
                regular((2,)),
                dma((PER,)),
                dma((4, PER)),
                dma((2, W)),
                dma((4,)),
                dma((4,)),
                dma,
                dma((2, 3)),
                dma((2, 2)),
                dma((4,)),
                dma((8,)),
            ],
            compiler_params=pltpu.CompilerParams(collective_id=0, has_side_effects=True, vmem_limit_bytes=40 * 2**20),
            cost_estimate=pl.CostEstimate(flops=10**9, bytes_accessed=3 * 10**8, transcendentals=3 * 2**20),
        )(*arrays)

    all_of, cut = P(None, None, None), P(None, "dp", None)
    return jax.shard_map(
        step,
        mesh=mesh,
        in_specs=(P(("rep", "dp"), None, None, None),) * 3 + (all_of,) * 3 + (cut,) * 6,
        out_specs=(P("rep", None, None),) * 3 + (P("rep", "dp", None),) * 6,
        check_vma=False,
    )
```

```python
import functools
import math

import jax
import jax.numpy as jnp
from jax import lax
from jax.experimental import pallas as pl
from jax.experimental.pallas import tpu as pltpu
from jax.sharding import PartitionSpec as P

MESH = pl.DeviceIdType.MESH
CR, CC = 128, 1024
PER = 24
N = 2 * PER
S = 4
D = 2
W = 3
AHEAD = 3 * D
LAG = 3
X = 12
ROWS = 16


def by_array(i, fn):
    for a in range(3):
        @pl.when((i >= 8 * a) & (i < 8 * a + 8))
        def _():
            t = i - 8 * a
            fn(a, t // 4, t % 4)


def whole(ref, a, layer, q, dd, lead=()):
    if a < 2:
        return ref.at[(*lead, layer, pl.ds(pl.multiple_of(dd * 128, 128), CR), pl.ds(pl.multiple_of(q * CC, CC), CC))]
    return ref.at[(*lead, layer, pl.ds(pl.multiple_of(dd * 512 + q * 128, 128), CR), pl.ds(0, CC))]


def kernel(count, *refs):
    terms, weights, ms, vs = refs[0:3], refs[3:6], refs[6:9], refs[9:12]
    wo, mo, vo, tail = refs[12:15], refs[15:18], refs[18:21], refs[21]
    (own, par, up, snd, gbuf, acc, nrm, fac, mb, vb, wb, mq, vq,
     own_s, par_s, give_s, up_s, snd_s, par_c, up_c, g_s, w_s, out_s, pr_s, ps_s, loc_s, in_s, mv_s, n_s, ns_s) = refs[22:]

    d = lax.axis_index("dp")
    z, c = d // 2, d % 2
    right = z >= 2
    is_end = (z == 0) | (z == 3)
    is_in = (z == 1) | (z == 2)
    mine = jnp.where(right, 2, 1)
    end = jnp.where(right, 3, 0)
    other = 3 - mine
    far = 3 - end
    partner = d + 1 - 2 * c

    def dev(zz):
        return {"dp": 2 * zz + c}

    buddy = {"dp": partner}

    def block_of(s, b):
        return 2 + b if s == 0 else 1 - b

    def block(ref, a, layer, q):
        if a < 2:
            return ref.at[layer, pl.ds(0, CR), pl.ds(pl.multiple_of(q * CC, CC), CC)]
        return ref.at[layer, pl.ds(pl.multiple_of(q * 128, 128), CR), pl.ds(0, CC)]

    def wait(ref, sem):
        pltpu.make_async_copy(ref, ref, sem).wait()

    def remote(src, dst, ssem, rsem, to):
        return pltpu.make_async_remote_copy(src, dst, ssem, rsem, device_id=to, device_id_type=MESH)

    def start_own(s, j):
        slot = lax.rem(j, S)
        dd = 2 * block_of(s, j // PER) + c

        def go(a, layer, q):
            pltpu.make_async_copy(whole(terms[a], a, layer, q, dd, (0,)), own.at[s, slot], own_s.at[s, slot]).start()

        by_array(lax.rem(j, PER), go)

    def start_give(s, j):
        slot = lax.rem(j, S)
        dd = 2 * block_of(s, j // PER) + 1 - c

        def go(a, layer, q):
            remote(whole(terms[a], a, layer, q, dd, (0,)), par.at[s, slot], give_s.at[s, slot], par_s.at[s, slot], buddy).start()

        by_array(lax.rem(j, PER), go)

    for s in range(2):
        for j in range(S):
            start_own(s, jnp.int32(j))

    barrier = pltpu.get_barrier_semaphore()
    for k in range(1, 8):
        pl.semaphore_signal(barrier, inc=1, device_id={"dp": lax.rem(d + k, 8)}, device_id_type=MESH)
    pl.semaphore_wait(barrier, 7)

    for s in range(2):
        for j in range(S):
            start_give(s, jnp.int32(j))

    acc[...] = jnp.zeros_like(acc)

    def rows(fn):
        def go(r, carry):
            fn(pl.ds(pl.multiple_of(r * ROWS, ROWS), ROWS))
            return carry

        lax.fori_loop(0, CR // ROWS, go, 0)

    def f32(x):
        return x.astype(jnp.float32)

    def process(s, k):
        zz = z if s == 0 else 3 - z
        down = z + 1 if s == 0 else z - 1
        above = z - 1 if s == 0 else z + 1
        j = k - D * zz

        @pl.when((j >= 0) & (j < N))
        def _():
            slot = lax.rem(j, S)
            wait(own.at[s, slot], own_s.at[s, slot])
            wait(par.at[s, slot], par_s.at[s, slot])

            @pl.when((zz < 3) & (j >= S))
            def _():
                wait(snd.at[s, slot], snd_s.at[s, slot])

            @pl.when(zz == 0)
            def _():
                def add(r):
                    snd[s, slot, r, :] = (f32(own[s, slot, r, :]) + f32(par[s, slot, r, :])).astype(jnp.bfloat16)

                rows(add)

            @pl.when(zz > 0)
            def _():
                wait(up.at[s, slot], up_s.at[s, slot])

            @pl.when((zz > 0) & (zz < 3))
            def _():
                def add(r):
                    snd[s, slot, r, :] = (f32(up[s, slot, r, :]) + (f32(own[s, slot, r, :]) + f32(par[s, slot, r, :]))).astype(jnp.bfloat16)

                rows(add)

            @pl.when(zz == 3)
            def _():
                def add(r):
                    g = (f32(up[s, slot, r, :]) + (f32(own[s, slot, r, :]) + f32(par[s, slot, r, :]))).astype(jnp.bfloat16)
                    gbuf[j, r, :] = g
                    acc[...] += f32(g) * f32(g)

                rows(add)

            @pl.when(j < N - S)
            def _():
                pl.semaphore_signal(par_c.at[s], inc=1, device_id=buddy, device_id_type=MESH)

            @pl.when((zz > 0) & (j < N - S))
            def _():
                pl.semaphore_signal(up_c.at[s], inc=1, device_id=dev(above), device_id_type=MESH)

            @pl.when(j + S < N)
            def _():
                start_own(s, j + S)

            @pl.when(zz < 3)
            def _():
                @pl.when(j >= S)
                def _():
                    pl.semaphore_wait(up_c.at[s], 1)

                remote(snd.at[s, slot], up.at[s, slot], snd_s.at[s, slot], up_s.at[s, slot], dev(down)).start()

            @pl.when((j >= 1) & (j + S - 1 < N))
            def _():
                again = lax.rem(j + S - 1, S)
                pl.semaphore_wait(par_c.at[s], 1)
                wait(par.at[s, again], give_s.at[s, again])
                start_give(s, j + S - 1)

    def room(link, u):
        @pl.when(u >= W)
        def _():
            wait(gbuf.at[0], out_s.at[link, lax.rem(u, W)])

    def send_sum(u):
        room(0, u)
        remote(gbuf.at[u], gbuf.at[u], out_s.at[0, lax.rem(u, W)], g_s.at[u], dev(mine)).start()

    def step(k, carry):
        process(0, k)
        process(1, k)

        @pl.when(is_end & (k >= N))
        def _():
            send_sum(k - N)

        return carry

    lax.fori_loop(0, N + 3 * D, step, 0)

    def start_mvw(i):
        slot = lax.rem(i, 2)

        def go(a, layer, q):
            pltpu.make_async_copy(block(ms[a], a, layer, q), mb.at[slot], in_s.at[slot, 0]).start()
            pltpu.make_async_copy(block(vs[a], a, layer, q), vb.at[slot], in_s.at[slot, 1]).start()
            pltpu.make_async_copy(whole(weights[a], a, layer, q, d), wb.at[slot], in_s.at[slot, 2]).start()

        by_array(i, go)

    start_mvw(jnp.int32(0))

    slot_of = jnp.where(right, 2, 0) + c

    @pl.when(is_end)
    def _():
        part = acc[0:8, 0:128]
        for r in range(ROWS // 8):
            for q in range(CC // 128):
                if r + q:
                    part = part + acc[8 * r : 8 * r + 8, 128 * q : 128 * q + 128]
        nrm[slot_of] = part
        for k in range(1, 8):
            remote(nrm.at[slot_of], nrm.at[slot_of], ns_s.at[k], n_s.at[slot_of], {"dp": lax.rem(d + k, 8)}).start()

    for s in range(2):
        for q in range(S):
            wait(par.at[s, q], give_s.at[s, q])
        zz = z if s == 0 else 3 - z

        @pl.when(zz < 3)
        def _():
            for q in range(S):
                wait(snd.at[s, q], snd_s.at[s, q])

    for k in range(4):
        @pl.when(jnp.logical_not(is_end & (slot_of == k)))
        def _():
            wait(nrm.at[k], n_s.at[k])

    total = jnp.sum((nrm[0] + nrm[1]) + (nrm[2] + nrm[3]), keepdims=True)
    fac[...] = jnp.broadcast_to(jnp.minimum(1.0, 0.5 * lax.rsqrt(total / count + 1e-30)), fac.shape)

    base = jnp.where(is_end, PER, 0)

    def update(i):
        slot = lax.rem(i, 2)
        at = base + i

        @pl.when(i + 1 < PER)
        def _():
            start_mvw(i + 1)

        wait(mb.at[slot], in_s.at[slot, 0])
        wait(vb.at[slot], in_s.at[slot, 1])
        wait(wb.at[slot], in_s.at[slot, 2])

        @pl.when(i >= 2)
        def _():
            wait(mq.at[slot], mv_s.at[slot, 0])
            wait(vq.at[slot], mv_s.at[slot, 1])

        @pl.when(is_in)
        def _():
            wait(gbuf.at[i], g_s.at[i])

        def adam(r):
            g = f32(gbuf[at, r, :]) * fac[...]
            m = 0.9 * mb[slot, r, :] + 0.1 * g
            v = 0.95 * vb[slot, r, :] + 0.05 * g * g
            w = f32(wb[slot, r, :])
            mq[slot, r, :] = m
            vq[slot, r, :] = v
            gbuf[at, r, :] = (w - 0.02 * (m * lax.rsqrt(v + 1e-8) + 0.1 * w)).astype(jnp.bfloat16)

        rows(adam)

        @pl.when(is_in)
        def _():
            room(0, i)
            room(1, i)

        def go(a, layer, q):
            new = gbuf.at[at]
            there = whole(wo[a], a, layer, q, d)
            pltpu.make_async_copy(mq.at[slot], block(mo[a], a, layer, q), mv_s.at[slot, 0]).start()
            pltpu.make_async_copy(vq.at[slot], block(vo[a], a, layer, q), mv_s.at[slot, 1]).start()

            @pl.when(is_in)
            def _():
                remote(new, there, out_s.at[0, lax.rem(i, W)], w_s.at[z, i], dev(end)).start()
                remote(new, there, out_s.at[1, lax.rem(i, W)], w_s.at[z, i], dev(other)).start()

            remote(new, there, ps_s.at[z], pr_s.at[z], buddy).start()
            pltpu.make_async_copy(new, there, loc_s).start()

        by_array(i, go)

    def send_new(i, u):
        room(0, u)

        def go(a, layer, q):
            remote(gbuf.at[PER + i], whole(wo[a], a, layer, q, d), out_s.at[0, lax.rem(u, W)], w_s.at[z, i], dev(mine)).start()

        by_array(i, go)

    def pass_on(i, src, over):
        if over is not None:
            room(over[0], over[1])

        def go(a, layer, q):
            here = whole(wo[a], a, layer, q, 2 * src + c)
            wait(here, w_s.at[src, i])
            if over is not None:
                sems = out_s.at[over[0], lax.rem(over[1], W)], w_s.at[src, i]
                if over[0] == 0:
                    remote(here, here, *sems, dev(over[2])).start()
                else:
                    @pl.when(i < PER - X)
                    def _():
                        remote(here, here, *sems, dev(over[2])).start()

                    @pl.when(i >= PER - X)
                    def _():
                        remote(here, tail.at[jnp.maximum(i - (PER - X), 0)], *sems, dev(over[2])).start()

            remote(here, here, ps_s.at[src], pr_s.at[src], buddy).start()

        by_array(i, go)

    def pass_tail(i):
        def go(a, layer, q):
            here = tail.at[i - (PER - X)]
            wait(here, w_s.at[far, i])
            remote(here, whole(wo[a], a, layer, q, 2 * far + c), ps_s.at[far], pr_s.at[far], buddy).start()

        by_array(i, go)

    @pl.when(is_in)
    def _():
        def first(t, carry):
            update(t)
            return carry

        lax.fori_loop(0, PER, first, 0)

        def second(i, carry):
            pass_on(i, other, (0, PER + i, end))
            pass_on(i, end, (1, PER + i, other))
            return carry

        lax.fori_loop(0, PER, second, 0)

        def third(i, carry):
            pass_on(i, far, (0, 2 * PER + i, end))
            return carry

        lax.fori_loop(0, PER - X, third, 0)

        def fourth(i, carry):
            pass_tail(i)
            return carry

        lax.fori_loop(PER - X, PER, fourth, 0)

    @pl.when(is_end)
    def _():
        def tick(t, carry):
            u = t + AHEAD

            @pl.when(u < PER)
            def _():
                send_sum(u)

            @pl.when(t < PER)
            def _():
                update(t)

            @pl.when((u >= PER) & (u < 2 * PER))
            def _():
                send_new(u - PER, u)

            got = t - LAG

            @pl.when((got >= 0) & (got < 3 * PER - X))
            def _():
                which = got // PER
                pass_on(lax.rem(got, PER), jnp.where(which == 0, mine, jnp.where(which == 1, other, far)), None)

            return carry

        lax.fori_loop(0, 3 * PER - X + LAG, tick, 0)

    for slot in range(2):
        wait(mq.at[slot], mv_s.at[slot, 0])
        wait(vq.at[slot], mv_s.at[slot, 1])
    six = gbuf.at[pl.ds(0, PER)]
    wait(six, loc_s)
    for k in range(W):
        wait(gbuf.at[0], out_s.at[0, k])

    @pl.when(is_in)
    def _():
        for k in range(W):
            wait(gbuf.at[0], out_s.at[1, k])

    @pl.when(is_end)
    def _():
        for k in range(1, 8):
            wait(nrm.at[slot_of], ns_s.at[k])

    for k in range(4):
        less = is_end & (far == k)

        @pl.when(less)
        def _():
            part = gbuf.at[pl.ds(0, PER - X)]
            wait(part, ps_s.at[k])
            wait(part, pr_s.at[k])

        @pl.when(jnp.logical_not(less))
        def _():
            wait(six, ps_s.at[k])
            wait(six, pr_s.at[k])


def copies(*refs):
    src, dst, buf, sem_in, sem_out = refs[0:9], refs[9:18], refs[18:22], refs[22], refs[23]
    items = []
    for a in range(9):
        down, layers, rows_ = a % 3 == 2, src[a].shape[0], src[a].shape[1]
        kind = (1 if down else 0) + (0 if a < 3 else 2)
        size = buf[kind].shape[1]
        items += [(a, kind, layer, r, size) for layer in range(layers) for r in range(0, rows_, size)]
    n = len(items)
    used = [[0] * 4, []]
    slots = []
    for it in items:
        slots.append(used[0][it[1]] % 3)
        used[0][it[1]] += 1
    last = {}

    def start_in(k):
        a, kind, layer, r, size = items[k]
        key = (kind, slots[k])
        if key in last:
            out(last[key]).wait()
        last[key] = k
        inn(k).start()

    def inn(k):
        a, kind, layer, r, size = items[k]
        return pltpu.make_async_copy(src[a].at[layer, pl.ds(r, size)], buf[kind].at[slots[k]], sem_in.at[kind, slots[k]])

    def out(k):
        a, kind, layer, r, size = items[k]
        return pltpu.make_async_copy(buf[kind].at[slots[k]], dst[a].at[layer, pl.ds(r, size)], sem_out.at[kind, slots[k]])

    for k in range(2):
        start_in(k)
    for k in range(n):
        inn(k).wait()
        out(k).start()
        if k + 2 < n:
            start_in(k + 2)
    for k in last.values():
        out(k).wait()


def place(tail, one, two, *refs):
    dst, buf, sem_in, sem_out = refs[3:6], refs[6], refs[7], refs[8]
    d = lax.axis_index("dp")
    z, c = d // 2, d % 2
    is_in = (z == 1) | (z == 2)
    far = jnp.where(z >= 2, 0, 3)

    @pl.when(is_in)
    def _():
        pltpu.make_async_copy(tail, buf.at[0], sem_in.at[0]).start()

    @pl.when(jnp.logical_not(is_in))
    def _():
        pltpu.make_async_copy(one, buf.at[0], sem_in.at[0]).start()
        pltpu.make_async_copy(two, buf.at[1], sem_in.at[1]).start()

    def put(which, core):
        pltpu.make_async_copy(one, buf.at[which], sem_in.at[which]).wait()
        for k in range(X):
            i = PER - X + k
            a = i // 8
            there = whole(dst[a], a, (i % 8) // 4, i % 4, 2 * far + core)
            pltpu.make_async_copy(buf.at[which, k], there, sem_out.at[which]).start()

    put(0, c)

    @pl.when(jnp.logical_not(is_in))
    def _():
        put(1, 1 - c)
        pltpu.make_async_copy(one, buf.at[1], sem_out.at[1]).wait()

    pltpu.make_async_copy(one, buf.at[0], sem_out.at[0]).wait()


def solution(mesh):
    def step(*arrays):
        weights, m = arrays[3:6], arrays[6:9]
        count = float(8 * sum(math.prod(a.shape) for a in m))
        any_ = pl.BlockSpec(memory_space=pl.ANY)
        chunk = (CR, CC)
        dma, regular = pltpu.SemaphoreType.DMA, pltpu.SemaphoreType.REGULAR
        out = [jax.ShapeDtypeStruct(w.shape, jnp.bfloat16) for w in weights] + [jax.ShapeDtypeStruct(a.shape, jnp.float32) for a in m] * 2
        last = jax.ShapeDtypeStruct((X, *chunk), jnp.bfloat16)
        *first, tail = pl.pallas_call(
            functools.partial(kernel, count),
            out_shape=[*out, last],
            in_specs=[any_] * 12,
            out_specs=[any_] * 10,
            scratch_shapes=[
                pltpu.VMEM((2, S, *chunk), jnp.bfloat16),
                pltpu.VMEM((2, S, *chunk), jnp.bfloat16),
                pltpu.VMEM((2, S, *chunk), jnp.bfloat16),
                pltpu.VMEM((2, S, *chunk), jnp.bfloat16),
                pltpu.VMEM((N, *chunk), jnp.bfloat16),
                pltpu.VMEM((ROWS, CC), jnp.float32),
                pltpu.VMEM((4, 8, 128), jnp.float32),
                pltpu.VMEM((1, CC), jnp.float32),
                pltpu.VMEM((2, *chunk), jnp.float32),
                pltpu.VMEM((2, *chunk), jnp.float32),
                pltpu.VMEM((2, *chunk), jnp.bfloat16),
                pltpu.VMEM((2, *chunk), jnp.float32),
                pltpu.VMEM((2, *chunk), jnp.float32),
                dma((2, S)),
                dma((2, S)),
                dma((2, S)),
                dma((2, S)),
                dma((2, S)),
                regular((2,)),
                regular((2,)),
                dma((PER,)),
                dma((4, PER)),
                dma((2, W)),
                dma((4,)),
                dma((4,)),
                dma,
                dma((2, 3)),
                dma((2, 2)),
                dma((4,)),
                dma((8,)),
            ],
            compiler_params=pltpu.CompilerParams(collective_id=0, has_side_effects=True, vmem_limit_bytes=40 * 2**20),
            cost_estimate=pl.CostEstimate(flops=10**9, bytes_accessed=3 * 10**8, transcendentals=3 * 2**20),
        )(*arrays)
        one = lax.ppermute(tail, "dp", [(2, 0), (3, 1), (4, 6), (5, 7)])
        copied = pl.pallas_call(
            copies,
            out_shape=out,
            in_specs=[any_] * 9,
            out_specs=[any_] * 9,
            scratch_shapes=[
                pltpu.VMEM((3, 256, 4096), jnp.bfloat16),
                pltpu.VMEM((3, 1024, 1024), jnp.bfloat16),
                pltpu.VMEM((3, 128, 4096), jnp.float32),
                pltpu.VMEM((3, 512, 1024), jnp.float32),
                dma((4, 3)),
                dma((4, 3)),
            ],
            compiler_params=pltpu.CompilerParams(vmem_limit_bytes=32 * 2**20),
            cost_estimate=pl.CostEstimate(flops=4 * 10**8, bytes_accessed=150 * 2**20, transcendentals=0),
        )(*first)
        one, *copied = lax.optimization_barrier((one, *copied))
        two = lax.ppermute(one, "dp", [(0, 1), (1, 0), (6, 7), (7, 6)])
        new = pl.pallas_call(
            place,
            out_shape=out[:3],
            in_specs=[any_] * 6,
            out_specs=[any_] * 3,
            input_output_aliases={3: 0, 4: 1, 5: 2},
            scratch_shapes=[pltpu.VMEM((2, X, *chunk), jnp.bfloat16), dma((2,)), dma((2,))],
            compiler_params=pltpu.CompilerParams(vmem_limit_bytes=16 * 2**20),
        )(tail, one, two, *copied[:3])
        return (*new, *copied[3:])

    all_of, cut = P(None, None, None), P(None, "dp", None)
    return jax.shard_map(
        step,
        mesh=mesh,
        in_specs=(P(("rep", "dp"), None, None, None),) * 3 + (all_of,) * 3 + (cut,) * 6,
        out_specs=(P("rep", None, None),) * 3 + (P("rep", "dp", None),) * 6,
        check_vma=False,
    )
```

```python
import functools
import math

import jax
import jax.numpy as jnp
from jax import lax
from jax.experimental import pallas as pl
from jax.experimental.pallas import tpu as pltpu
from jax.sharding import PartitionSpec as P

MESH = pl.DeviceIdType.MESH
CR, CC = 128, 1024
PER = 24
N = 2 * PER
S = 4
LOCAL = 8
GUEST = PER - LOCAL
D = 2
W = 3
AHEAD = 2 * D
LAG = 3
X = 8
ROWS = 16


def by_array(i, fn):
    for a in range(3):
        @pl.when((i >= 8 * a) & (i < 8 * a + 8))
        def _():
            t = i - 8 * a
            fn(a, t // 4, t % 4)


def whole(ref, a, layer, q, dd, lead=()):
    if a < 2:
        return ref.at[(*lead, layer, pl.ds(pl.multiple_of(dd * 128, 128), CR), pl.ds(pl.multiple_of(q * CC, CC), CC))]
    return ref.at[(*lead, layer, pl.ds(pl.multiple_of(dd * 512 + q * 128, 128), CR), pl.ds(0, CC))]


def kernel(count, *refs):
    terms, weights, ms, vs = refs[0:3], refs[3:6], refs[6:9], refs[9:12]
    wo, mo, vo, tail = refs[12:15], refs[15:18], refs[18:21], refs[21]
    (own, par, up, snd, ext, pre, gbuf, acc, nrm, fac, mb, vb, wb, mq, vq,
     own_s, par_s, give_s, up_s, snd_s, par_c, up_c, g_s, ext_s, pre_s, pf_s, w_s, out_s, pr_s, ps_s, loc_s, in_s, mv_s, n_s, ns_s) = refs[22:]

    d, group = lax.axis_index("dp"), lax.axis_index("rep")
    z, c = d // 2, d % 2
    right = z >= 2
    is_end = (z == 0) | (z == 3)
    is_in = (z == 1) | (z == 2)
    mine = jnp.where(right, 2, 1)
    end = jnp.where(right, 3, 0)
    other = 3 - mine
    far = 3 - end
    partner = d + 1 - 2 * c

    def dev(zz):
        return {"dp": 2 * zz + c}

    buddy = {"dp": partner}

    def chunk_of(s, n):
        zz = z if s == 0 else 3 - z
        m = jnp.where(zz == 3, jnp.where(n < 4, N - LOCAL + n, jnp.where(n < N - 4, n - 4, n)), n)
        late = m >= N - LOCAL
        b = jnp.where((m >= GUEST) & jnp.logical_not(late), 1, 0)
        i = jnp.where(late, m - (N - PER), m - b * GUEST)
        return (2 + b if s == 0 else 1 - b), b, i

    def block(ref, a, layer, q):
        if a < 2:
            return ref.at[layer, pl.ds(0, CR), pl.ds(pl.multiple_of(q * CC, CC), CC)]
        return ref.at[layer, pl.ds(pl.multiple_of(q * 128, 128), CR), pl.ds(0, CC)]

    def wait(ref, sem):
        pltpu.make_async_copy(ref, ref, sem).wait()

    def remote(src, dst, ssem, rsem, to):
        return pltpu.make_async_remote_copy(src, dst, ssem, rsem, device_id=to, device_id_type=MESH)

    def start_own(s, j):
        slot = lax.rem(j, S)
        home, _, i = chunk_of(s, j)
        dd = 2 * home + c

        def go(a, layer, q):
            pltpu.make_async_copy(whole(terms[a], a, layer, q, dd, (0,)), own.at[s, slot], own_s.at[s, slot]).start()

        by_array(i, go)

    def start_give(s, j):
        slot = lax.rem(j, S)
        home, _, i = chunk_of(s, j)
        dd = 2 * home + 1 - c

        def go(a, layer, q):
            remote(whole(terms[a], a, layer, q, dd, (0,)), par.at[s, slot], give_s.at[s, slot], par_s.at[s, slot], buddy).start()

        by_array(i, go)

    for s in range(2):
        for j in range(S):
            start_own(s, jnp.int32(j))

    barrier = pltpu.get_barrier_semaphore()
    for k in range(1, 8):
        pl.semaphore_signal(barrier, inc=1, device_id={"dp": lax.rem(d + k, 8)}, device_id_type=MESH)
    for k in range(1, 4):
        pl.semaphore_signal(barrier, inc=1, device_id={"rep": lax.rem(group + k, 4)}, device_id_type=MESH)
    pl.semaphore_wait(barrier, 10)

    for s in range(2):
        for j in range(S):
            start_give(s, jnp.int32(j))

    acc[...] = jnp.zeros_like(acc)

    def rows(fn):
        def go(r, carry):
            fn(pl.ds(pl.multiple_of(r * ROWS, ROWS), ROWS))
            return carry

        lax.fori_loop(0, CR // ROWS, go, 0)

    def f32(x):
        return x.astype(jnp.float32)

    def process(s, k):
        zz = z if s == 0 else 3 - z
        down = z + 1 if s == 0 else z - 1
        above = z - 1 if s == 0 else z + 1
        j = k - jnp.where(zz == 3, 3 * D - 4, D * zz)

        @pl.when((j >= 0) & (j < N))
        def _():
            slot = lax.rem(j, S)
            _, b, i = chunk_of(s, j)
            back = (zz == 3) & ((j < 4) | (j >= N - 4))
            here = (zz == 2) & (j >= N - LOCAL)
            root = (zz == 3) & jnp.logical_not(back)
            on = (zz < 3) & jnp.logical_not(here)
            wait(own.at[s, slot], own_s.at[s, slot])
            wait(par.at[s, slot], par_s.at[s, slot])

            @pl.when((on & (j >= S)) | (back & (j >= N - 4)))
            def _():
                wait(snd.at[s, slot], snd_s.at[s, slot])

            @pl.when((zz > 0) & jnp.logical_not(back))
            def _():
                wait(up.at[s, slot], up_s.at[s, slot])

            def two(r):
                return f32(own[s, slot, r, :]) + f32(par[s, slot, r, :])

            @pl.when((zz == 0) | back)
            def _():
                def add(r):
                    snd[s, slot, r, :] = two(r).astype(jnp.bfloat16)

                rows(add)

            @pl.when((zz > 0) & on)
            def _():
                def add(r):
                    snd[s, slot, r, :] = (f32(up[s, slot, r, :]) + two(r)).astype(jnp.bfloat16)

                rows(add)

            def keep(r, total):
                g = total.astype(jnp.bfloat16)
                gbuf[b * PER + i, r, :] = g
                acc[...] += f32(g) * f32(g)

            @pl.when(root)
            def _():
                rows(lambda r: keep(r, f32(up[s, slot, r, :]) + two(r)))

            @pl.when(here)
            def _():
                e = i - GUEST
                wait(ext.at[e], ext_s.at[e])
                rows(lambda r: keep(r, f32(up[s, slot, r, :]) + two(r) + f32(ext[e, r, :])))

            @pl.when(j < N - S)
            def _():
                pl.semaphore_signal(par_c.at[s], inc=1, device_id=buddy, device_id_type=MESH)

            @pl.when(((zz > 0) & (zz < 3) & (j < N - S)) | (root & (j < N - LOCAL + 4 - S)))
            def _():
                pl.semaphore_signal(up_c.at[s], inc=1, device_id=dev(above), device_id_type=MESH)

            @pl.when(j + S < N)
            def _():
                start_own(s, j + S)

            @pl.when(on)
            def _():
                @pl.when(j >= S)
                def _():
                    pl.semaphore_wait(up_c.at[s], 1)

                remote(snd.at[s, slot], up.at[s, slot], snd_s.at[s, slot], up_s.at[s, slot], dev(down)).start()

            @pl.when(back)
            def _():
                e = jnp.maximum(i - GUEST, 0)
                remote(snd.at[s, slot], ext.at[e], snd_s.at[s, slot], ext_s.at[e], dev(above)).start()

            @pl.when((j >= 1) & (j + S - 1 < N))
            def _():
                again = lax.rem(j + S - 1, S)
                pl.semaphore_wait(par_c.at[s], 1)
                wait(par.at[s, again], give_s.at[s, again])
                start_give(s, j + S - 1)

    def bring(h):
        i, kind = 4 * (h // 2) + group, lax.rem(h, 2)

        def go(a, layer, q):
            for which, ref in enumerate((ms[a], vs[a])):
                @pl.when(kind == which)
                def _():
                    remote(block(ref, a, layer, q), pre.at[i, which], pf_s, pre_s.at[i, which], dev(end)).start()

        by_array(i, go)

    def share(h):
        i, kind = 4 * (h // 2) + group, lax.rem(h, 2)
        wait(pre.at[i, kind], pre_s.at[i, kind])
        for k in range(1, 4):
            remote(pre.at[i, kind], pre.at[i, kind], pf_s, pre_s.at[i, kind], {"rep": lax.rem(group + k, 4)}).start()

    def room(link, u):
        @pl.when(u >= W)
        def _():
            wait(gbuf.at[0], out_s.at[link, lax.rem(u, W)])

    def send_sum(u):
        room(0, u)
        remote(gbuf.at[u], gbuf.at[u], out_s.at[0, lax.rem(u, W)], g_s.at[u], dev(mine)).start()

    def step(k, carry):
        @pl.when(is_in & (k < 4))
        def _():
            bring(k)

        process(0, k)
        process(1, k)

        @pl.when(is_in & (k >= N - 4) & (k < N))
        def _():
            bring(k - (N - 8))

        @pl.when(is_end & (k >= 4) & (k < 8))
        def _():
            share(k - 4)

        @pl.when(is_end & (k >= N))
        def _():
            send_sum(k - N)

        return carry

    lax.fori_loop(0, N + 2 * D, step, 0)

    def order(t):
        return jnp.where(t < LOCAL, GUEST + t, t - LOCAL)

    def start_mvw(t, i):
        slot = lax.rem(t, 2)

        def go(a, layer, q):
            pltpu.make_async_copy(block(ms[a], a, layer, q), mb.at[slot], in_s.at[slot, 0]).start()
            pltpu.make_async_copy(block(vs[a], a, layer, q), vb.at[slot], in_s.at[slot, 1]).start()
            pltpu.make_async_copy(whole(weights[a], a, layer, q, d), wb.at[slot], in_s.at[slot, 2]).start()

        by_array(i, go)

    start_mvw(jnp.int32(0), jnp.where(is_end, 0, GUEST))

    part = acc[0:8, 0:128]
    for r in range(ROWS // 8):
        for q in range(CC // 128):
            if r + q:
                part = part + acc[8 * r : 8 * r + 8, 128 * q : 128 * q + 128]
    nrm[d] = part
    for k in range(1, 8):
        remote(nrm.at[d], nrm.at[d], ns_s.at[k], n_s.at[d], {"dp": lax.rem(d + k, 8)}).start()

    for s in range(2):
        for q in range(S):
            wait(par.at[s, q], give_s.at[s, q])
        for q in range(S):
            wait(snd.at[s, q], snd_s.at[s, q])

    for k in range(8):
        @pl.when(d != k)
        def _():
            wait(nrm.at[k], n_s.at[k])

    total = ((nrm[0] + nrm[1]) + (nrm[2] + nrm[3])) + ((nrm[4] + nrm[5]) + (nrm[6] + nrm[7]))
    total = jnp.sum(total, keepdims=True)
    fac[...] = jnp.broadcast_to(jnp.minimum(1.0, 0.5 * lax.rsqrt(total / count + 1e-30)), fac.shape)

    base = jnp.where(is_end, PER, 0)

    def start_guest(t):
        slot = lax.rem(t, 2)

        def go(a, layer, q):
            pltpu.make_async_copy(whole(weights[a], a, layer, q, 2 * mine + c), wb.at[slot], in_s.at[slot, 2]).start()

        by_array(t - PER, go)

    def adam(g, m, v, w):
        g = f32(g) * fac[...]
        m = 0.9 * m + 0.1 * g
        v = 0.95 * v + 0.05 * g * g
        w = f32(w)
        return m, v, (w - 0.02 * (m * lax.rsqrt(v + 1e-8) + 0.1 * w)).astype(jnp.bfloat16)

    def update(t, i):
        slot = lax.rem(t, 2)
        at = base + i

        @pl.when(t + 1 < PER)
        def _():
            start_mvw(t + 1, jnp.where(is_end, i + 1, order(t + 1)))

        @pl.when(is_end & (t + 1 == PER))
        def _():
            start_guest(t + 1)

        wait(mb.at[slot], in_s.at[slot, 0])
        wait(vb.at[slot], in_s.at[slot, 1])
        wait(wb.at[slot], in_s.at[slot, 2])

        @pl.when(t >= 2)
        def _():
            wait(mq.at[slot], mv_s.at[slot, 0])
            wait(vq.at[slot], mv_s.at[slot, 1])

        @pl.when(is_in & (i < GUEST))
        def _():
            wait(gbuf.at[i], g_s.at[i])

        def new_rows(r):
            m, v, w = adam(gbuf[at, r, :], mb[slot, r, :], vb[slot, r, :], wb[slot, r, :])
            mq[slot, r, :] = m
            vq[slot, r, :] = v
            gbuf[at, r, :] = w

        rows(new_rows)

        @pl.when(is_in)
        def _():
            room(1, t)

        @pl.when(is_in & (t < LOCAL))
        def _():
            room(0, t)

        def go(a, layer, q):
            new = gbuf.at[at]
            there = whole(wo[a], a, layer, q, d)
            pltpu.make_async_copy(mq.at[slot], block(mo[a], a, layer, q), mv_s.at[slot, 0]).start()
            pltpu.make_async_copy(vq.at[slot], block(vo[a], a, layer, q), mv_s.at[slot, 1]).start()

            @pl.when(is_in)
            def _():
                remote(new, there, out_s.at[1, lax.rem(t, W)], w_s.at[z, i], dev(other)).start()

            @pl.when(is_in & (t < LOCAL))
            def _():
                remote(new, there, out_s.at[0, lax.rem(t, W)], w_s.at[z, i], dev(end)).start()

            remote(new, there, ps_s.at[z], pr_s.at[z], buddy).start()
            pltpu.make_async_copy(new, there, loc_s).start()

        by_array(i, go)

    def update_guest(t):
        slot = lax.rem(t, 2)
        i = t - PER

        @pl.when(t + 1 < PER + GUEST)
        def _():
            start_guest(t + 1)

        wait(wb.at[slot], in_s.at[slot, 2])

        @pl.when(lax.rem(i, 4) != group)
        def _():
            wait(pre.at[i, 0], pre_s.at[i, 0])
            wait(pre.at[i, 1], pre_s.at[i, 1])

        def new_rows(r):
            gbuf[i, r, :] = adam(gbuf[i, r, :], pre[i, 0, r, :], pre[i, 1, r, :], wb[slot, r, :])[2]

        rows(new_rows)

        def go(a, layer, q):
            new = gbuf.at[i]
            there = whole(wo[a], a, layer, q, 2 * mine + c)
            remote(new, there, ps_s.at[mine], pr_s.at[mine], buddy).start()
            pltpu.make_async_copy(new, there, loc_s).start()

        by_array(i, go)

    def send_new(i, u):
        room(0, u)

        def go(a, layer, q):
            remote(gbuf.at[PER + i], whole(wo[a], a, layer, q, d), out_s.at[0, lax.rem(u, W)], w_s.at[z, i], dev(mine)).start()

        by_array(i, go)

    def pass_on(i, src, over):
        if over is not None:
            room(over[0], over[1])

        def go(a, layer, q):
            here = whole(wo[a], a, layer, q, 2 * src + c)
            wait(here, w_s.at[src, i])
            if over is not None:
                sems = out_s.at[over[0], lax.rem(over[1], W)], w_s.at[src, i]
                if over[0] == 0:
                    remote(here, here, *sems, dev(over[2])).start()
                else:
                    @pl.when(i < PER - X)
                    def _():
                        remote(here, here, *sems, dev(over[2])).start()

                    @pl.when(i >= PER - X)
                    def _():
                        remote(here, tail.at[jnp.maximum(i - (PER - X), 0)], *sems, dev(over[2])).start()

            remote(here, here, ps_s.at[src], pr_s.at[src], buddy).start()

        by_array(i, go)

    def pass_tail(i):
        def go(a, layer, q):
            here = tail.at[i - (PER - X)]
            wait(here, w_s.at[far, i])
            remote(here, whole(wo[a], a, layer, q, 2 * far + c), ps_s.at[far], pr_s.at[far], buddy).start()

        by_array(i, go)

    @pl.when(is_in)
    def _():
        def tick(t, carry):
            @pl.when(t < PER)
            def _():
                update(t, order(t))

            @pl.when((t >= LOCAL) & (t < LOCAL + PER))
            def _():
                pass_on(order(t - LOCAL), other, (0, t, end))

            @pl.when((t >= PER) & (t < 2 * PER))
            def _():
                pass_on(t - PER, end, (1, t, other))

            f = t - (LOCAL + PER)

            @pl.when((f >= 0) & (f < PER - X))
            def _():
                pass_on(f, far, (0, t, end))

            @pl.when(f >= PER - X)
            def _():
                pass_tail(f)

            return carry

        lax.fori_loop(0, LOCAL + 2 * PER, tick, 0)

    @pl.when(is_end)
    def _():
        def tick(t, carry):
            u = t + AHEAD

            @pl.when(u < GUEST)
            def _():
                send_sum(u)

            @pl.when(t < 4)
            def _():
                share(4 + t)

            @pl.when(t < PER)
            def _():
                update(t, t)

            @pl.when((u >= GUEST) & (u < GUEST + PER))
            def _():
                send_new(u - GUEST, u)

            @pl.when((t >= PER) & (t < PER + GUEST))
            def _():
                update_guest(t)

            got = t - LAG

            @pl.when((got >= 0) & (got < LOCAL + 2 * PER - X))
            def _():
                src = jnp.where(got < LOCAL, mine, jnp.where(got < LOCAL + PER, other, far))
                i = jnp.where(got < LOCAL, GUEST + got, jnp.where(got < LOCAL + PER, order(got - LOCAL), got - LOCAL - PER))
                pass_on(i, src, None)

            return carry

        lax.fori_loop(0, LOCAL + 2 * PER - X + LAG, tick, 0)

    for slot in range(2):
        wait(mq.at[slot], mv_s.at[slot, 0])
        wait(vq.at[slot], mv_s.at[slot, 1])
    six = gbuf.at[pl.ds(0, PER)]
    for k in range(W):
        wait(gbuf.at[0], out_s.at[0, k])

    @pl.when(is_in)
    def _():
        wait(six, loc_s)
        wait(gbuf.at[pl.ds(0, 16)], pf_s)
        for k in range(W):
            wait(gbuf.at[0], out_s.at[1, k])

    @pl.when(is_end)
    def _():
        wait(gbuf.at[pl.ds(0, PER + GUEST)], loc_s)
        wait(gbuf.at[pl.ds(0, 48)], pf_s)

    for k in range(1, 8):
        wait(nrm.at[d], ns_s.at[k])

    for k in range(4):
        less = is_end & (far == k)

        @pl.when(less)
        def _():
            part = gbuf.at[pl.ds(0, PER - X)]
            wait(part, ps_s.at[k])
            wait(part, pr_s.at[k])

        @pl.when(jnp.logical_not(less))
        def _():
            wait(six, ps_s.at[k])
            wait(six, pr_s.at[k])


def copies(*refs):
    src, dst, buf, sem_in, sem_out = refs[0:9], refs[9:18], refs[18:22], refs[22], refs[23]
    items = []
    for a in range(9):
        down, layers, rows_ = a % 3 == 2, src[a].shape[0], src[a].shape[1]
        kind = (1 if down else 0) + (0 if a < 3 else 2)
        size = buf[kind].shape[1]
        items += [(a, kind, layer, r, size) for layer in range(layers) for r in range(0, rows_, size)]
    n = len(items)
    used = [[0] * 4, []]
    slots = []
    for it in items:
        slots.append(used[0][it[1]] % 3)
        used[0][it[1]] += 1
    last = {}

    def start_in(k):
        a, kind, layer, r, size = items[k]
        key = (kind, slots[k])
        if key in last:
            out(last[key]).wait()
        last[key] = k
        inn(k).start()

    def inn(k):
        a, kind, layer, r, size = items[k]
        return pltpu.make_async_copy(src[a].at[layer, pl.ds(r, size)], buf[kind].at[slots[k]], sem_in.at[kind, slots[k]])

    def out(k):
        a, kind, layer, r, size = items[k]
        return pltpu.make_async_copy(buf[kind].at[slots[k]], dst[a].at[layer, pl.ds(r, size)], sem_out.at[kind, slots[k]])

    for k in range(2):
        start_in(k)
    for k in range(n):
        inn(k).wait()
        out(k).start()
        if k + 2 < n:
            start_in(k + 2)
    for k in last.values():
        out(k).wait()


def place(tail, one, two, *refs):
    dst, buf, sem_in, sem_out = refs[3:6], refs[6], refs[7], refs[8]
    d = lax.axis_index("dp")
    z, c = d // 2, d % 2
    is_in = (z == 1) | (z == 2)
    far = jnp.where(z >= 2, 0, 3)

    @pl.when(is_in)
    def _():
        pltpu.make_async_copy(tail, buf.at[0], sem_in.at[0]).start()

    @pl.when(jnp.logical_not(is_in))
    def _():
        pltpu.make_async_copy(one, buf.at[0], sem_in.at[0]).start()
        pltpu.make_async_copy(two, buf.at[1], sem_in.at[1]).start()

    def put(which, core):
        pltpu.make_async_copy(one, buf.at[which], sem_in.at[which]).wait()
        for k in range(X):
            i = PER - X + k
            a = i // 8
            there = whole(dst[a], a, (i % 8) // 4, i % 4, 2 * far + core)
            pltpu.make_async_copy(buf.at[which, k], there, sem_out.at[which]).start()

    put(0, c)

    @pl.when(jnp.logical_not(is_in))
    def _():
        put(1, 1 - c)
        pltpu.make_async_copy(one, buf.at[1], sem_out.at[1]).wait()

    pltpu.make_async_copy(one, buf.at[0], sem_out.at[0]).wait()


def solution(mesh):
    def step(*arrays):
        weights, m = arrays[3:6], arrays[6:9]
        count = float(8 * sum(math.prod(a.shape) for a in m))
        any_ = pl.BlockSpec(memory_space=pl.ANY)
        chunk = (CR, CC)
        dma, regular = pltpu.SemaphoreType.DMA, pltpu.SemaphoreType.REGULAR
        out = [jax.ShapeDtypeStruct(w.shape, jnp.bfloat16) for w in weights] + [jax.ShapeDtypeStruct(a.shape, jnp.float32) for a in m] * 2
        last = jax.ShapeDtypeStruct((X, *chunk), jnp.bfloat16)
        *first, tail = pl.pallas_call(
            functools.partial(kernel, count),
            out_shape=[*out, last],
            in_specs=[any_] * 12,
            out_specs=[any_] * 10,
            scratch_shapes=[
                pltpu.VMEM((2, S, *chunk), jnp.bfloat16),
                pltpu.VMEM((2, S, *chunk), jnp.bfloat16),
                pltpu.VMEM((2, S, *chunk), jnp.bfloat16),
                pltpu.VMEM((2, S, *chunk), jnp.bfloat16),
                pltpu.VMEM((LOCAL, *chunk), jnp.bfloat16),
                pltpu.VMEM((GUEST, 2, *chunk), jnp.float32),
                pltpu.VMEM((N, *chunk), jnp.bfloat16),
                pltpu.VMEM((ROWS, CC), jnp.float32),
                pltpu.VMEM((8, 8, 128), jnp.float32),
                pltpu.VMEM((1, CC), jnp.float32),
                pltpu.VMEM((2, *chunk), jnp.float32),
                pltpu.VMEM((2, *chunk), jnp.float32),
                pltpu.VMEM((2, *chunk), jnp.bfloat16),
                pltpu.VMEM((2, *chunk), jnp.float32),
                pltpu.VMEM((2, *chunk), jnp.float32),
                dma((2, S)),
                dma((2, S)),
                dma((2, S)),
                dma((2, S)),
                dma((2, S)),
                regular((2,)),
                regular((2,)),
                dma((PER,)),
                dma((LOCAL,)),
                dma((GUEST, 2)),
                dma,
                dma((4, PER)),
                dma((2, W)),
                dma((4,)),
                dma((4,)),
                dma,
                dma((2, 3)),
                dma((2, 2)),
                dma((8,)),
                dma((8,)),
            ],
            compiler_params=pltpu.CompilerParams(collective_id=0, has_side_effects=True, vmem_limit_bytes=54 * 2**20),
            cost_estimate=pl.CostEstimate(flops=10**9, bytes_accessed=3 * 10**8, transcendentals=3 * 2**20),
        )(*arrays)
        one = lax.ppermute(tail, "dp", [(2, 0), (3, 1), (4, 6), (5, 7)])
        copied = pl.pallas_call(
            copies,
            out_shape=out,
            in_specs=[any_] * 9,
            out_specs=[any_] * 9,
            scratch_shapes=[
                pltpu.VMEM((3, 256, 4096), jnp.bfloat16),
                pltpu.VMEM((3, 1024, 1024), jnp.bfloat16),
                pltpu.VMEM((3, 128, 4096), jnp.float32),
                pltpu.VMEM((3, 512, 1024), jnp.float32),
                dma((4, 3)),
                dma((4, 3)),
            ],
            compiler_params=pltpu.CompilerParams(vmem_limit_bytes=32 * 2**20),
            cost_estimate=pl.CostEstimate(flops=4 * 10**8, bytes_accessed=150 * 2**20, transcendentals=0),
        )(*first)
        one, *copied = lax.optimization_barrier((one, *copied))
        two = lax.ppermute(one, "dp", [(0, 1), (1, 0), (6, 7), (7, 6)])
        new = pl.pallas_call(
            place,
            out_shape=out[:3],
            in_specs=[any_] * 6,
            out_specs=[any_] * 3,
            input_output_aliases={3: 0, 4: 1, 5: 2},
            scratch_shapes=[pltpu.VMEM((2, X, *chunk), jnp.bfloat16), dma((2,)), dma((2,))],
            compiler_params=pltpu.CompilerParams(vmem_limit_bytes=16 * 2**20),
        )(tail, one, two, *copied[:3])
        return (*new, *copied[3:])

    all_of, cut = P(None, None, None), P(None, "dp", None)
    return jax.shard_map(
        step,
        mesh=mesh,
        in_specs=(P(("rep", "dp"), None, None, None),) * 3 + (all_of,) * 3 + (cut,) * 6,
        out_specs=(P("rep", None, None),) * 3 + (P("rep", "dp", None),) * 6,
        check_vma=False,
    )
```

```python
import functools
import math

import jax
import jax.numpy as jnp
from jax import lax
from jax.experimental import pallas as pl
from jax.experimental.pallas import tpu as pltpu
from jax.sharding import PartitionSpec as P

MESH = pl.DeviceIdType.MESH
CR, CC = 128, 1024
PER = 24
N = 2 * PER
S = 4
U = 8
LOCAL = 8
GUEST = PER - LOCAL
D = 2
W = 3
PAUSE = D + 2
STEPS = N + 2 * D + PAUSE
AHEAD = 2
LAG = 3
COPIES, LOOK = 6, 4
X = 8
ROWS = 16


def by_array(i, fn):
    for a in range(3):
        @pl.when((i >= 8 * a) & (i < 8 * a + 8))
        def _():
            t = i - 8 * a
            fn(a, t // 4, t % 4)


def whole(ref, a, layer, q, dd, lead=()):
    if a < 2:
        return ref.at[(*lead, layer, pl.ds(pl.multiple_of(dd * 128, 128), CR), pl.ds(pl.multiple_of(q * CC, CC), CC))]
    return ref.at[(*lead, layer, pl.ds(pl.multiple_of(dd * 512 + q * 128, 128), CR), pl.ds(0, CC))]


def kernel(count, *refs):
    terms, weights, ms, vs = refs[0:3], refs[3:6], refs[6:9], refs[9:12]
    wo, mo, vo, tail = refs[12:15], refs[15:18], refs[18:21], refs[21]
    (own, par, up, snd, ext, pre, gbuf, acc, nrm, fac, mb, vb, wb, mq, vq,
     own_s, par_s, give_s, up_s, snd_s, par_c, up_c, g_s, ext_s, pre_s, pf_s, w_s, out_s, pr_s, ps_s, loc_s, in_s, mv_s, n_s, ns_s) = refs[22:]

    d, group = lax.axis_index("dp"), lax.axis_index("rep")
    z, c = d // 2, d % 2
    right = z >= 2
    is_end = (z == 0) | (z == 3)
    is_in = (z == 1) | (z == 2)
    mine = jnp.where(right, 2, 1)
    end = jnp.where(right, 3, 0)
    other = 3 - mine
    far = 3 - end
    partner = d + 1 - 2 * c

    def dev(zz):
        return {"dp": 2 * zz + c}

    buddy = {"dp": partner}

    def chunk_of(s, n):
        late = n >= N - LOCAL
        b = jnp.where((n >= GUEST) & jnp.logical_not(late), 1, 0)
        i = jnp.where(late, n - (N - PER), n - b * GUEST)
        return (2 + b if s == 0 else 1 - b), b, i

    def block(ref, a, layer, q):
        if a < 2:
            return ref.at[layer, pl.ds(0, CR), pl.ds(pl.multiple_of(q * CC, CC), CC)]
        return ref.at[layer, pl.ds(pl.multiple_of(q * 128, 128), CR), pl.ds(0, CC)]

    def wait(ref, sem):
        pltpu.make_async_copy(ref, ref, sem).wait()

    def remote(src, dst, ssem, rsem, to):
        return pltpu.make_async_remote_copy(src, dst, ssem, rsem, device_id=to, device_id_type=MESH)

    def start_own(s, j):
        slot = lax.rem(j, S)
        home, _, i = chunk_of(s, j)
        dd = 2 * home + c

        def go(a, layer, q):
            pltpu.make_async_copy(whole(terms[a], a, layer, q, dd, (0,)), own.at[s, slot], own_s.at[s, slot]).start()

        by_array(i, go)

    def start_give(s, j):
        slot = lax.rem(j, S)
        home, _, i = chunk_of(s, j)
        dd = 2 * home + 1 - c

        def go(a, layer, q):
            remote(whole(terms[a], a, layer, q, dd, (0,)), par.at[s, slot], give_s.at[s, slot], par_s.at[s, slot], buddy).start()

        by_array(i, go)

    for s in range(2):
        for j in range(S):
            start_own(s, jnp.int32(j))

    barrier = pltpu.get_barrier_semaphore()
    for k in range(1, 8):
        pl.semaphore_signal(barrier, inc=1, device_id={"dp": lax.rem(d + k, 8)}, device_id_type=MESH)
    for k in range(1, 4):
        pl.semaphore_signal(barrier, inc=1, device_id={"rep": lax.rem(group + k, 4)}, device_id_type=MESH)
    pl.semaphore_wait(barrier, 10)

    for s in range(2):
        for j in range(S):
            start_give(s, jnp.int32(j))

    acc[...] = jnp.zeros_like(acc)

    def rows(fn):
        def go(r, carry):
            fn(pl.ds(pl.multiple_of(r * ROWS, ROWS), ROWS))
            return carry

        lax.fori_loop(0, CR // ROWS, go, 0)

    def f32(x):
        return x.astype(jnp.float32)

    def process(s, k):
        zz = z if s == 0 else 3 - z
        down = z + 1 if s == 0 else z - 1
        above = z - 1 if s == 0 else z + 1
        j = k - D * zz
        pause = (zz == 2) & (j >= N - LOCAL)
        held = pause & (j < N - LOCAL + PAUSE)
        j = j - jnp.where(pause, PAUSE, 0)

        @pl.when((j >= 0) & (j < N) & jnp.logical_not(held))
        def _():
            slot, place_ = lax.rem(j, S), lax.rem(j, U)
            _, b, i = chunk_of(s, j)
            back = (zz == 3) & (j >= N - LOCAL)
            here = (zz == 2) & (j >= N - LOCAL)
            root = (zz == 3) & jnp.logical_not(back)
            on = (zz < 3) & jnp.logical_not(here)
            wait(own.at[s, slot], own_s.at[s, slot])
            wait(par.at[s, slot], par_s.at[s, slot])

            @pl.when((on & (j >= S)) | (back & (j >= N - LOCAL + S)))
            def _():
                wait(snd.at[s, slot], snd_s.at[s, slot])

            @pl.when((zz > 0) & jnp.logical_not(back))
            def _():
                wait(up.at[s, place_], up_s.at[s, place_])

            def two(r):
                return f32(own[s, slot, r, :]) + f32(par[s, slot, r, :])

            @pl.when((zz == 0) | back)
            def _():
                def add(r):
                    snd[s, slot, r, :] = two(r).astype(jnp.bfloat16)

                rows(add)

            @pl.when((zz > 0) & on)
            def _():
                def add(r):
                    snd[s, slot, r, :] = (f32(up[s, place_, r, :]) + two(r)).astype(jnp.bfloat16)

                rows(add)

            def keep(r, total):
                g = total.astype(jnp.bfloat16)
                gbuf[b * PER + i, r, :] = g
                acc[...] += f32(g) * f32(g)

            @pl.when(root)
            def _():
                rows(lambda r: keep(r, f32(up[s, place_, r, :]) + two(r)))

            @pl.when(here)
            def _():
                e = i - GUEST
                wait(ext.at[e], ext_s.at[e])
                rows(lambda r: keep(r, f32(up[s, place_, r, :]) + two(r) + f32(ext[e, r, :])))

            @pl.when(j < N - S)
            def _():
                pl.semaphore_signal(par_c.at[s], inc=1, device_id=buddy, device_id_type=MESH)

            @pl.when(((zz > 0) & (zz < 3) & (j < N - U)) | (root & (j < N - LOCAL - U)))
            def _():
                pl.semaphore_signal(up_c.at[s], inc=1, device_id=dev(above), device_id_type=MESH)

            @pl.when(j + S < N)
            def _():
                start_own(s, j + S)

            @pl.when(on)
            def _():
                @pl.when(j >= U)
                def _():
                    pl.semaphore_wait(up_c.at[s], 1)

                remote(snd.at[s, slot], up.at[s, place_], snd_s.at[s, slot], up_s.at[s, place_], dev(down)).start()

            @pl.when(back)
            def _():
                e = jnp.maximum(i - GUEST, 0)
                remote(snd.at[s, slot], ext.at[e], snd_s.at[s, slot], ext_s.at[e], dev(above)).start()

            @pl.when((j >= 1) & (j + S - 1 < N))
            def _():
                again = lax.rem(j + S - 1, S)
                pl.semaphore_wait(par_c.at[s], 1)
                wait(par.at[s, again], give_s.at[s, again])
                start_give(s, j + S - 1)

    def bring(h):
        i, kind = 4 * (h // 2) + group, lax.rem(h, 2)

        def go(a, layer, q):
            for which, ref in enumerate((ms[a], vs[a])):
                @pl.when(kind == which)
                def _():
                    remote(block(ref, a, layer, q), pre.at[i, which], pf_s, pre_s.at[i, which], dev(end)).start()

        by_array(i, go)

    def share(h):
        i, kind = 4 * (h // 2) + group, lax.rem(h, 2)
        wait(pre.at[i, kind], pre_s.at[i, kind])
        for k in range(1, 4):
            remote(pre.at[i, kind], pre.at[i, kind], pf_s, pre_s.at[i, kind], {"rep": lax.rem(group + k, 4)}).start()

    def room(link, u):
        @pl.when(u >= W)
        def _():
            wait(gbuf.at[0], out_s.at[link, lax.rem(u, W)])

    def send_sum(u):
        room(0, u)
        remote(gbuf.at[u], gbuf.at[u], out_s.at[0, lax.rem(u, W)], g_s.at[u], dev(mine)).start()

    def step(k, carry):
        @pl.when(is_in & (k < 2))
        def _():
            bring(k)

        process(0, k)
        process(1, k)

        @pl.when(is_in & (k >= N - 4) & (k < N + 2))
        def _():
            bring(k - (N - 6))

        @pl.when(is_end & ((k == 6) | (k == 7)))
        def _():
            share(k - 6)

        @pl.when(is_end & (k >= STEPS - AHEAD))
        def _():
            send_sum(k - (STEPS - AHEAD))

        return carry

    lax.fori_loop(0, STEPS, step, 0)

    def order(t):
        return jnp.where(t < LOCAL, GUEST + t, t - LOCAL)

    def start_mvw(t, i):
        slot = lax.rem(t, 2)

        def go(a, layer, q):
            pltpu.make_async_copy(block(ms[a], a, layer, q), mb.at[slot], in_s.at[slot, 0]).start()
            pltpu.make_async_copy(block(vs[a], a, layer, q), vb.at[slot], in_s.at[slot, 1]).start()
            pltpu.make_async_copy(whole(weights[a], a, layer, q, d), wb.at[slot], in_s.at[slot, 2]).start()

        by_array(i, go)

    start_mvw(jnp.int32(0), jnp.where(is_end, 0, GUEST))

    part = acc[0:8, 0:128]
    for r in range(ROWS // 8):
        for q in range(CC // 128):
            if r + q:
                part = part + acc[8 * r : 8 * r + 8, 128 * q : 128 * q + 128]
    nrm[d] = part
    for k in range(1, 8):
        remote(nrm.at[d], nrm.at[d], ns_s.at[k], n_s.at[d], {"dp": lax.rem(d + k, 8)}).start()

    for s in range(2):
        for q in range(S):
            wait(par.at[s, q], give_s.at[s, q])
        for q in range(S):
            wait(snd.at[s, q], snd_s.at[s, q])

    for k in range(8):
        @pl.when(d != k)
        def _():
            wait(nrm.at[k], n_s.at[k])

    total = ((nrm[0] + nrm[1]) + (nrm[2] + nrm[3])) + ((nrm[4] + nrm[5]) + (nrm[6] + nrm[7]))
    total = jnp.sum(total, keepdims=True)
    fac[...] = jnp.broadcast_to(jnp.minimum(1.0, 0.5 * lax.rsqrt(total / count + 1e-30)), fac.shape)

    base = jnp.where(is_end, PER, 0)

    def start_guest(t):
        slot = lax.rem(t, 2)

        def go(a, layer, q):
            pltpu.make_async_copy(whole(weights[a], a, layer, q, 2 * mine + c), wb.at[slot], in_s.at[slot, 2]).start()

        by_array(t - PER, go)

    def adam(g, m, v, w):
        g = f32(g) * fac[...]
        m = 0.9 * m + 0.1 * g
        v = 0.95 * v + 0.05 * g * g
        w = f32(w)
        return m, v, (w - 0.02 * (m * lax.rsqrt(v + 1e-8) + 0.1 * w)).astype(jnp.bfloat16)

    def update(t, i):
        slot = lax.rem(t, 2)
        at = base + i

        @pl.when(t + 1 < PER)
        def _():
            start_mvw(t + 1, jnp.where(is_end, i + 1, order(t + 1)))

        @pl.when(is_end & (t + 1 == PER))
        def _():
            start_guest(t + 1)

        wait(mb.at[slot], in_s.at[slot, 0])
        wait(vb.at[slot], in_s.at[slot, 1])
        wait(wb.at[slot], in_s.at[slot, 2])

        @pl.when(t >= 2)
        def _():
            wait(mq.at[slot], mv_s.at[slot, 0])
            wait(vq.at[slot], mv_s.at[slot, 1])

        @pl.when(is_in & (i < GUEST))
        def _():
            wait(gbuf.at[i], g_s.at[i])

        def new_rows(r):
            m, v, w = adam(gbuf[at, r, :], mb[slot, r, :], vb[slot, r, :], wb[slot, r, :])
            mq[slot, r, :] = m
            vq[slot, r, :] = v
            gbuf[at, r, :] = w

        rows(new_rows)

        @pl.when(is_in)
        def _():
            room(1, t)

        @pl.when(is_in & (t < LOCAL))
        def _():
            room(0, t)

        def go(a, layer, q):
            new = gbuf.at[at]
            there = whole(wo[a], a, layer, q, d)
            pltpu.make_async_copy(mq.at[slot], block(mo[a], a, layer, q), mv_s.at[slot, 0]).start()
            pltpu.make_async_copy(vq.at[slot], block(vo[a], a, layer, q), mv_s.at[slot, 1]).start()

            @pl.when(is_in)
            def _():
                remote(new, there, out_s.at[1, lax.rem(t, W)], w_s.at[z, i], dev(other)).start()

            @pl.when(is_in & (t < LOCAL))
            def _():
                remote(new, there, out_s.at[0, lax.rem(t, W)], w_s.at[z, i], dev(end)).start()

            remote(new, there, ps_s.at[z], pr_s.at[z], buddy).start()
            pltpu.make_async_copy(new, there, loc_s).start()

        by_array(i, go)

    def update_guest(t):
        slot = lax.rem(t, 2)
        i = t - PER

        @pl.when(t + 1 < PER + GUEST)
        def _():
            start_guest(t + 1)

        wait(wb.at[slot], in_s.at[slot, 2])

        @pl.when(lax.rem(i, 4) != group)
        def _():
            wait(pre.at[i, 0], pre_s.at[i, 0])
            wait(pre.at[i, 1], pre_s.at[i, 1])

        def new_rows(r):
            gbuf[i, r, :] = adam(gbuf[i, r, :], pre[i, 0, r, :], pre[i, 1, r, :], wb[slot, r, :])[2]

        rows(new_rows)

        def go(a, layer, q):
            new = gbuf.at[i]
            there = whole(wo[a], a, layer, q, 2 * mine + c)
            remote(new, there, ps_s.at[mine], pr_s.at[mine], buddy).start()
            pltpu.make_async_copy(new, there, loc_s).start()

        by_array(i, go)

    def send_new(i, u):
        room(0, u)

        def go(a, layer, q):
            remote(gbuf.at[PER + i], whole(wo[a], a, layer, q, d), out_s.at[0, lax.rem(u, W)], w_s.at[z, i], dev(mine)).start()

        by_array(i, go)

    def pass_on(i, src, over):
        if over is not None:
            room(over[0], over[1])

        def go(a, layer, q):
            here = whole(wo[a], a, layer, q, 2 * src + c)
            wait(here, w_s.at[src, i])
            if over is not None:
                sems = out_s.at[over[0], lax.rem(over[1], W)], w_s.at[src, i]
                if over[0] == 0:
                    remote(here, here, *sems, dev(over[2])).start()
                else:
                    @pl.when(i < PER - X)
                    def _():
                        remote(here, here, *sems, dev(over[2])).start()

                    @pl.when(i >= PER - X)
                    def _():
                        remote(here, tail.at[jnp.maximum(i - (PER - X), 0)], *sems, dev(over[2])).start()

            remote(here, here, ps_s.at[src], pr_s.at[src], buddy).start()

        by_array(i, go)

    def pass_tail(i):
        def go(a, layer, q):
            here = tail.at[i - (PER - X)]
            wait(here, w_s.at[far, i])
            remote(here, whole(wo[a], a, layer, q, 2 * far + c), ps_s.at[far], pr_s.at[far], buddy).start()

        by_array(i, go)

    @pl.when(is_in)
    def _():
        def tick(t, carry):
            @pl.when(t < PER)
            def _():
                update(t, order(t))

            @pl.when((t >= LOCAL) & (t < LOCAL + PER))
            def _():
                pass_on(order(t - LOCAL), other, (0, t, end))

            @pl.when((t >= PER) & (t < 2 * PER))
            def _():
                pass_on(t - PER, end, (1, t, other))

            f = t - (LOCAL + PER)

            @pl.when((f >= 0) & (f < PER - X))
            def _():
                pass_on(f, far, (0, t, end))

            @pl.when(f >= PER - X)
            def _():
                pass_tail(f)

            return carry

        lax.fori_loop(0, LOCAL + 2 * PER, tick, 0)

    @pl.when(is_end)
    def _():
        def tick(t, carry):
            u = t + AHEAD

            @pl.when(u < GUEST)
            def _():
                send_sum(u)

            @pl.when(t < 6)
            def _():
                share(2 + t)

            @pl.when(t < PER)
            def _():
                update(t, t)

            @pl.when((u >= GUEST) & (u < GUEST + PER))
            def _():
                send_new(u - GUEST, u)

            @pl.when((t >= PER) & (t < PER + GUEST))
            def _():
                update_guest(t)

            got = t - LAG

            @pl.when((got >= 0) & (got < LOCAL + 2 * PER - X))
            def _():
                src = jnp.where(got < LOCAL, mine, jnp.where(got < LOCAL + PER, other, far))
                i = jnp.where(got < LOCAL, GUEST + got, jnp.where(got < LOCAL + PER, order(got - LOCAL), got - LOCAL - PER))
                pass_on(i, src, None)

            return carry

        lax.fori_loop(0, LOCAL + 2 * PER - X + LAG, tick, 0)

    for slot in range(2):
        wait(mq.at[slot], mv_s.at[slot, 0])
        wait(vq.at[slot], mv_s.at[slot, 1])
    six = gbuf.at[pl.ds(0, PER)]
    for k in range(W):
        wait(gbuf.at[0], out_s.at[0, k])

    @pl.when(is_in)
    def _():
        wait(six, loc_s)
        wait(gbuf.at[pl.ds(0, 16)], pf_s)
        for k in range(W):
            wait(gbuf.at[0], out_s.at[1, k])

    @pl.when(is_end)
    def _():
        wait(gbuf.at[pl.ds(0, PER + GUEST)], loc_s)
        wait(gbuf.at[pl.ds(0, 48)], pf_s)

    for k in range(1, 8):
        wait(nrm.at[d], ns_s.at[k])

    for k in range(4):
        less = is_end & (far == k)

        @pl.when(less)
        def _():
            part = gbuf.at[pl.ds(0, PER - X)]
            wait(part, ps_s.at[k])
            wait(part, pr_s.at[k])

        @pl.when(jnp.logical_not(less))
        def _():
            wait(six, ps_s.at[k])
            wait(six, pr_s.at[k])


def copies(*refs):
    src, dst, buf, sem_in, sem_out = refs[0:9], refs[9:18], refs[18:22], refs[22], refs[23]
    items = []
    for a in range(9):
        down, layers, rows_ = a % 3 == 2, src[a].shape[0], src[a].shape[1]
        kind = (1 if down else 0) + (0 if a < 3 else 2)
        size = buf[kind].shape[1]
        items += [(a, kind, layer, r, size) for layer in range(layers) for r in range(0, rows_, size)]
    n = len(items)
    used = [[0] * 4, []]
    slots = []
    for it in items:
        slots.append(used[0][it[1]] % COPIES)
        used[0][it[1]] += 1
    last = {}

    def start_in(k):
        a, kind, layer, r, size = items[k]
        key = (kind, slots[k])
        if key in last:
            out(last[key]).wait()
        last[key] = k
        inn(k).start()

    def inn(k):
        a, kind, layer, r, size = items[k]
        return pltpu.make_async_copy(src[a].at[layer, pl.ds(r, size)], buf[kind].at[slots[k]], sem_in.at[kind, slots[k]])

    def out(k):
        a, kind, layer, r, size = items[k]
        return pltpu.make_async_copy(buf[kind].at[slots[k]], dst[a].at[layer, pl.ds(r, size)], sem_out.at[kind, slots[k]])

    for k in range(LOOK):
        start_in(k)
    for k in range(n):
        inn(k).wait()
        out(k).start()
        if k + LOOK < n:
            start_in(k + LOOK)
    for k in last.values():
        out(k).wait()


def place(tail, one, two, *refs):
    dst, buf, sem_in, sem_out = refs[3:6], refs[6], refs[7], refs[8]
    d = lax.axis_index("dp")
    z, c = d // 2, d % 2
    is_in = (z == 1) | (z == 2)
    far = jnp.where(z >= 2, 0, 3)

    @pl.when(is_in)
    def _():
        pltpu.make_async_copy(tail, buf.at[0], sem_in.at[0]).start()

    @pl.when(jnp.logical_not(is_in))
    def _():
        pltpu.make_async_copy(one, buf.at[0], sem_in.at[0]).start()
        pltpu.make_async_copy(two, buf.at[1], sem_in.at[1]).start()

    def put(which, core):
        pltpu.make_async_copy(one, buf.at[which], sem_in.at[which]).wait()
        for k in range(X):
            i = PER - X + k
            a = i // 8
            there = whole(dst[a], a, (i % 8) // 4, i % 4, 2 * far + core)
            pltpu.make_async_copy(buf.at[which, k], there, sem_out.at[which]).start()

    put(0, c)

    @pl.when(jnp.logical_not(is_in))
    def _():
        put(1, 1 - c)
        pltpu.make_async_copy(one, buf.at[1], sem_out.at[1]).wait()

    pltpu.make_async_copy(one, buf.at[0], sem_out.at[0]).wait()


def solution(mesh):
    def step(*arrays):
        weights, m = arrays[3:6], arrays[6:9]
        count = float(8 * sum(math.prod(a.shape) for a in m))
        any_ = pl.BlockSpec(memory_space=pl.ANY)
        chunk = (CR, CC)
        dma, regular = pltpu.SemaphoreType.DMA, pltpu.SemaphoreType.REGULAR
        out = [jax.ShapeDtypeStruct(w.shape, jnp.bfloat16) for w in weights] + [jax.ShapeDtypeStruct(a.shape, jnp.float32) for a in m] * 2
        last = jax.ShapeDtypeStruct((X, *chunk), jnp.bfloat16)
        *first, tail = pl.pallas_call(
            functools.partial(kernel, count),
            out_shape=[*out, last],
            in_specs=[any_] * 12,
            out_specs=[any_] * 10,
            scratch_shapes=[
                pltpu.VMEM((2, S, *chunk), jnp.bfloat16),
                pltpu.VMEM((2, S, *chunk), jnp.bfloat16),
                pltpu.VMEM((2, U, *chunk), jnp.bfloat16),
                pltpu.VMEM((2, S, *chunk), jnp.bfloat16),
                pltpu.VMEM((LOCAL, *chunk), jnp.bfloat16),
                pltpu.VMEM((GUEST, 2, *chunk), jnp.float32),
                pltpu.VMEM((N, *chunk), jnp.bfloat16),
                pltpu.VMEM((ROWS, CC), jnp.float32),
                pltpu.VMEM((8, 8, 128), jnp.float32),
                pltpu.VMEM((1, CC), jnp.float32),
                pltpu.VMEM((2, *chunk), jnp.float32),
                pltpu.VMEM((2, *chunk), jnp.float32),
                pltpu.VMEM((2, *chunk), jnp.bfloat16),
                pltpu.VMEM((2, *chunk), jnp.float32),
                pltpu.VMEM((2, *chunk), jnp.float32),
                dma((2, S)),
                dma((2, S)),
                dma((2, S)),
                dma((2, U)),
                dma((2, S)),
                regular((2,)),
                regular((2,)),
                dma((PER,)),
                dma((LOCAL,)),
                dma((GUEST, 2)),
                dma,
                dma((4, PER)),
                dma((2, W)),
                dma((4,)),
                dma((4,)),
                dma,
                dma((2, 3)),
                dma((2, 2)),
                dma((8,)),
                dma((8,)),
            ],
            compiler_params=pltpu.CompilerParams(collective_id=0, has_side_effects=True, vmem_limit_bytes=54 * 2**20),
            cost_estimate=pl.CostEstimate(flops=10**9, bytes_accessed=3 * 10**8, transcendentals=3 * 2**20),
        )(*arrays)
        one = lax.ppermute(tail, "dp", [(2, 0), (3, 1), (4, 6), (5, 7)])
        copied = pl.pallas_call(
            copies,
            out_shape=out,
            in_specs=[any_] * 9,
            out_specs=[any_] * 9,
            scratch_shapes=[
                pltpu.VMEM((COPIES, 256, 4096), jnp.bfloat16),
                pltpu.VMEM((COPIES, 1024, 1024), jnp.bfloat16),
                pltpu.VMEM((COPIES, 128, 4096), jnp.float32),
                pltpu.VMEM((COPIES, 512, 1024), jnp.float32),
                dma((4, COPIES)),
                dma((4, COPIES)),
            ],
            compiler_params=pltpu.CompilerParams(vmem_limit_bytes=63 * 2**20),
            cost_estimate=pl.CostEstimate(flops=4 * 10**8, bytes_accessed=150 * 2**20, transcendentals=0),
        )(*first)
        one, *copied = lax.optimization_barrier((one, *copied))
        two = lax.ppermute(one, "dp", [(0, 1), (1, 0), (6, 7), (7, 6)])
        new = pl.pallas_call(
            place,
            out_shape=out[:3],
            in_specs=[any_] * 6,
            out_specs=[any_] * 3,
            input_output_aliases={3: 0, 4: 1, 5: 2},
            scratch_shapes=[pltpu.VMEM((2, X, *chunk), jnp.bfloat16), dma((2,)), dma((2,))],
            compiler_params=pltpu.CompilerParams(vmem_limit_bytes=16 * 2**20),
        )(tail, one, two, *copied[:3])
        return (*new, *copied[3:])

    all_of, cut = P(None, None, None), P(None, "dp", None)
    return jax.shard_map(
        step,
        mesh=mesh,
        in_specs=(P(("rep", "dp"), None, None, None),) * 3 + (all_of,) * 3 + (cut,) * 6,
        out_specs=(P("rep", None, None),) * 3 + (P("rep", "dp", None),) * 6,
        check_vma=False,
    )
```

```python
import functools
import math

import jax
import jax.numpy as jnp
from jax import lax
from jax.experimental import pallas as pl
from jax.experimental.pallas import tpu as pltpu
from jax.sharding import PartitionSpec as P

MESH = pl.DeviceIdType.MESH
CR, CC = 128, 1024
PER = 24
N = 2 * PER
S = 4
U = 8
LOCAL = 8
GUEST = PER - LOCAL
D = 2
W = 3
PAUSE = D + 2
STEPS = N + 2 * D + PAUSE
AHEAD = 2
LAG = 3
COPIES, LOOK = 6, 4
X = 8
ROWS = 16


def by_array(i, fn):
    for a in range(3):
        @pl.when((i >= 8 * a) & (i < 8 * a + 8))
        def _():
            t = i - 8 * a
            fn(a, t // 4, t % 4)


def whole(ref, a, layer, q, dd, lead=()):
    if a < 2:
        return ref.at[(*lead, layer, pl.ds(pl.multiple_of(dd * 128, 128), CR), pl.ds(pl.multiple_of(q * CC, CC), CC))]
    return ref.at[(*lead, layer, pl.ds(pl.multiple_of(dd * 512 + q * 128, 128), CR), pl.ds(0, CC))]


def kernel(count, *refs):
    terms, weights, ms, vs = refs[0:3], refs[3:6], refs[6:9], refs[9:12]
    wo, mo, vo, tail = refs[12:15], refs[15:18], refs[18:21], refs[21]
    (own, par, up, snd, ext, pre, gbuf, acc, nrm, fac, mb, vb, wb, mq, vq,
     own_s, par_s, give_s, up_s, snd_s, par_c, up_c, g_s, ext_s, pre_s, pf_s, w_s, out_s, pr_s, ps_s, loc_s, in_s, mv_s, n_s, ns_s) = refs[22:]

    d, group = lax.axis_index("dp"), lax.axis_index("rep")
    z, c = d // 2, d % 2
    right = z >= 2
    is_end = (z == 0) | (z == 3)
    is_in = (z == 1) | (z == 2)
    mine = jnp.where(right, 2, 1)
    end = jnp.where(right, 3, 0)
    other = 3 - mine
    far = 3 - end
    partner = d + 1 - 2 * c

    def dev(zz):
        return {"dp": 2 * zz + c}

    buddy = {"dp": partner}

    def chunk_of(s, n):
        late = n >= N - LOCAL
        b = jnp.where((n >= GUEST) & jnp.logical_not(late), 1, 0)
        i = jnp.where(late, n - (N - PER), n - b * GUEST)
        return (2 + b if s == 0 else 1 - b), b, i

    def block(ref, a, layer, q):
        if a < 2:
            return ref.at[layer, pl.ds(0, CR), pl.ds(pl.multiple_of(q * CC, CC), CC)]
        return ref.at[layer, pl.ds(pl.multiple_of(q * 128, 128), CR), pl.ds(0, CC)]

    def wait(ref, sem):
        pltpu.make_async_copy(ref, ref, sem).wait()

    def remote(src, dst, ssem, rsem, to):
        return pltpu.make_async_remote_copy(src, dst, ssem, rsem, device_id=to, device_id_type=MESH)

    def start_own(s, j):
        slot = lax.rem(j, S)
        home, _, i = chunk_of(s, j)
        dd = 2 * home + c

        def go(a, layer, q):
            pltpu.make_async_copy(whole(terms[a], a, layer, q, dd, (0,)), own.at[s, slot], own_s.at[s, slot]).start()

        by_array(i, go)

    def start_give(s, j):
        slot = lax.rem(j, S)
        home, _, i = chunk_of(s, j)
        dd = 2 * home + 1 - c

        def go(a, layer, q):
            remote(whole(terms[a], a, layer, q, dd, (0,)), par.at[s, slot], give_s.at[s, slot], par_s.at[s, slot], buddy).start()

        by_array(i, go)

    for s in range(2):
        for j in range(S):
            start_own(s, jnp.int32(j))

    barrier = pltpu.get_barrier_semaphore()
    for k in range(1, 8):
        pl.semaphore_signal(barrier, inc=1, device_id={"dp": lax.rem(d + k, 8)}, device_id_type=MESH)
    for k in range(1, 4):
        pl.semaphore_signal(barrier, inc=1, device_id={"rep": lax.rem(group + k, 4)}, device_id_type=MESH)
    pl.semaphore_wait(barrier, 10)

    for s in range(2):
        start_give(s, jnp.int32(0))

    acc[...] = jnp.zeros_like(acc)

    def rows(fn):
        def go(r, carry):
            fn(pl.ds(pl.multiple_of(r * ROWS, ROWS), ROWS))
            return carry

        lax.fori_loop(0, CR // ROWS, go, 0)

    def f32(x):
        return x.astype(jnp.float32)

    def process(s, k):
        zz = z if s == 0 else 3 - z
        down = z + 1 if s == 0 else z - 1
        above = z - 1 if s == 0 else z + 1
        j = k - D * zz
        pause = (zz == 2) & (j >= N - LOCAL)
        held = pause & (j < N - LOCAL + PAUSE)
        j = j - jnp.where(pause, PAUSE, 0)

        @pl.when((j >= 0) & (j < N) & jnp.logical_not(held))
        def _():
            slot, place_ = lax.rem(j, S), lax.rem(j, U)
            _, b, i = chunk_of(s, j)
            back = (zz == 3) & (j >= N - LOCAL)
            here = (zz == 2) & (j >= N - LOCAL)
            root = (zz == 3) & jnp.logical_not(back)
            on = (zz < 3) & jnp.logical_not(here)
            wait(own.at[s, slot], own_s.at[s, slot])
            wait(par.at[s, slot], par_s.at[s, slot])

            @pl.when((on & (j >= S)) | (back & (j >= N - LOCAL + S)))
            def _():
                wait(snd.at[s, slot], snd_s.at[s, slot])

            @pl.when((zz > 0) & jnp.logical_not(back))
            def _():
                wait(up.at[s, place_], up_s.at[s, place_])

            def two(r):
                return f32(own[s, slot, r, :]) + f32(par[s, slot, r, :])

            @pl.when((zz == 0) | back)
            def _():
                def add(r):
                    snd[s, slot, r, :] = two(r).astype(jnp.bfloat16)

                rows(add)

            @pl.when((zz > 0) & on)
            def _():
                def add(r):
                    snd[s, slot, r, :] = (f32(up[s, place_, r, :]) + two(r)).astype(jnp.bfloat16)

                rows(add)

            def keep(r, total):
                g = total.astype(jnp.bfloat16)
                gbuf[b * PER + i, r, :] = g
                acc[...] += f32(g) * f32(g)

            @pl.when(root)
            def _():
                rows(lambda r: keep(r, f32(up[s, place_, r, :]) + two(r)))

            @pl.when(here)
            def _():
                e = i - GUEST
                wait(ext.at[e], ext_s.at[e])
                rows(lambda r: keep(r, f32(up[s, place_, r, :]) + two(r) + f32(ext[e, r, :])))

            @pl.when(j < N - S)
            def _():
                pl.semaphore_signal(par_c.at[s], inc=1, device_id=buddy, device_id_type=MESH)

            @pl.when(((zz > 0) & (zz < 3) & (j < N - U)) | (root & (j < N - LOCAL - U)))
            def _():
                pl.semaphore_signal(up_c.at[s], inc=1, device_id=dev(above), device_id_type=MESH)

            @pl.when(j + S < N)
            def _():
                start_own(s, j + S)

            @pl.when(on)
            def _():
                @pl.when(j >= U)
                def _():
                    pl.semaphore_wait(up_c.at[s], 1)

                remote(snd.at[s, slot], up.at[s, place_], snd_s.at[s, slot], up_s.at[s, place_], dev(down)).start()

            @pl.when(back)
            def _():
                e = jnp.maximum(i - GUEST, 0)
                remote(snd.at[s, slot], ext.at[e], snd_s.at[s, slot], ext_s.at[e], dev(above)).start()

            @pl.when((j >= 1) & (j + S - 1 < N))
            def _():
                again = lax.rem(j + S - 1, S)
                pl.semaphore_wait(par_c.at[s], 1)
                wait(par.at[s, again], give_s.at[s, again])
                start_give(s, j + S - 1)

    def bring(h):
        i, kind = 4 * (h // 2) + group, lax.rem(h, 2)

        def go(a, layer, q):
            for which, ref in enumerate((ms[a], vs[a])):
                @pl.when(kind == which)
                def _():
                    remote(block(ref, a, layer, q), pre.at[i, which], pf_s, pre_s.at[i, which], dev(end)).start()

        by_array(i, go)

    def share(h):
        i, kind = 4 * (h // 2) + group, lax.rem(h, 2)
        wait(pre.at[i, kind], pre_s.at[i, kind])
        for k in range(1, 4):
            remote(pre.at[i, kind], pre.at[i, kind], pf_s, pre_s.at[i, kind], {"rep": lax.rem(group + k, 4)}).start()

    def room(link, u):
        @pl.when(u >= W)
        def _():
            wait(gbuf.at[0], out_s.at[link, lax.rem(u, W)])

    def send_sum(u):
        room(0, u)
        remote(gbuf.at[u], gbuf.at[u], out_s.at[0, lax.rem(u, W)], g_s.at[u], dev(mine)).start()

    def step(k, carry):
        @pl.when(is_in & (k < 2))
        def _():
            bring(k)

        process(0, k)
        process(1, k)

        @pl.when(k == 0)
        def _():
            for s in range(2):
                for j in range(1, S):
                    start_give(s, jnp.int32(j))

        @pl.when(is_in & (k >= N - 4) & (k < N + 2))
        def _():
            bring(k - (N - 6))

        @pl.when(is_end & ((k == 6) | (k == 7)))
        def _():
            share(k - 6)

        @pl.when(is_end & (k >= STEPS - AHEAD))
        def _():
            send_sum(k - (STEPS - AHEAD))

        return carry

    lax.fori_loop(0, STEPS, step, 0)

    def order(t):
        return jnp.where(t < LOCAL, GUEST + t, t - LOCAL)

    def start_mvw(t, i):
        slot = lax.rem(t, 2)

        def go(a, layer, q):
            pltpu.make_async_copy(block(ms[a], a, layer, q), mb.at[slot], in_s.at[slot, 0]).start()
            pltpu.make_async_copy(block(vs[a], a, layer, q), vb.at[slot], in_s.at[slot, 1]).start()
            pltpu.make_async_copy(whole(weights[a], a, layer, q, d), wb.at[slot], in_s.at[slot, 2]).start()

        by_array(i, go)

    start_mvw(jnp.int32(0), jnp.where(is_end, 0, GUEST))

    part = acc[0:8, 0:128]
    for r in range(ROWS // 8):
        for q in range(CC // 128):
            if r + q:
                part = part + acc[8 * r : 8 * r + 8, 128 * q : 128 * q + 128]
    nrm[d] = part
    for k in range(1, 8):
        remote(nrm.at[d], nrm.at[d], ns_s.at[k], n_s.at[d], {"dp": lax.rem(d + k, 8)}).start()

    for s in range(2):
        for q in range(S):
            wait(par.at[s, q], give_s.at[s, q])
        for q in range(S):
            wait(snd.at[s, q], snd_s.at[s, q])

    for k in range(8):
        @pl.when(d != k)
        def _():
            wait(nrm.at[k], n_s.at[k])

    total = ((nrm[0] + nrm[1]) + (nrm[2] + nrm[3])) + ((nrm[4] + nrm[5]) + (nrm[6] + nrm[7]))
    total = jnp.sum(total, keepdims=True)
    fac[...] = jnp.broadcast_to(jnp.minimum(1.0, 0.5 * lax.rsqrt(total / count + 1e-30)), fac.shape)

    base = jnp.where(is_end, PER, 0)

    def start_guest(t):
        slot = lax.rem(t, 2)

        def go(a, layer, q):
            pltpu.make_async_copy(whole(weights[a], a, layer, q, 2 * mine + c), wb.at[slot], in_s.at[slot, 2]).start()

        by_array(t - PER, go)

    def adam(g, m, v, w):
        g = f32(g) * fac[...]
        m = 0.9 * m + 0.1 * g
        v = 0.95 * v + 0.05 * g * g
        w = f32(w)
        return m, v, (w - 0.02 * (m * lax.rsqrt(v + 1e-8) + 0.1 * w)).astype(jnp.bfloat16)

    def update(t, i):
        slot = lax.rem(t, 2)
        at = base + i

        @pl.when(t + 1 < PER)
        def _():
            start_mvw(t + 1, jnp.where(is_end, i + 1, order(t + 1)))

        @pl.when(is_end & (t + 1 == PER))
        def _():
            start_guest(t + 1)

        wait(mb.at[slot], in_s.at[slot, 0])
        wait(vb.at[slot], in_s.at[slot, 1])
        wait(wb.at[slot], in_s.at[slot, 2])

        @pl.when(t >= 2)
        def _():
            wait(mq.at[slot], mv_s.at[slot, 0])
            wait(vq.at[slot], mv_s.at[slot, 1])

        @pl.when(is_in & (i < GUEST))
        def _():
            wait(gbuf.at[i], g_s.at[i])

        def new_rows(r):
            m, v, w = adam(gbuf[at, r, :], mb[slot, r, :], vb[slot, r, :], wb[slot, r, :])
            mq[slot, r, :] = m
            vq[slot, r, :] = v
            gbuf[at, r, :] = w

        rows(new_rows)

        @pl.when(is_in)
        def _():
            room(1, t)

        @pl.when(is_in & (t < LOCAL))
        def _():
            room(0, t)

        def go(a, layer, q):
            new = gbuf.at[at]
            there = whole(wo[a], a, layer, q, d)
            pltpu.make_async_copy(mq.at[slot], block(mo[a], a, layer, q), mv_s.at[slot, 0]).start()
            pltpu.make_async_copy(vq.at[slot], block(vo[a], a, layer, q), mv_s.at[slot, 1]).start()

            @pl.when(is_in)
            def _():
                remote(new, there, out_s.at[1, lax.rem(t, W)], w_s.at[z, i], dev(other)).start()

            @pl.when(is_in & (t < LOCAL))
            def _():
                remote(new, there, out_s.at[0, lax.rem(t, W)], w_s.at[z, i], dev(end)).start()

            remote(new, there, ps_s.at[z], pr_s.at[z], buddy).start()
            pltpu.make_async_copy(new, there, loc_s).start()

        by_array(i, go)

    def update_guest(t):
        slot = lax.rem(t, 2)
        i = t - PER

        @pl.when(t + 1 < PER + GUEST)
        def _():
            start_guest(t + 1)

        wait(wb.at[slot], in_s.at[slot, 2])

        @pl.when(lax.rem(i, 4) != group)
        def _():
            wait(pre.at[i, 0], pre_s.at[i, 0])
            wait(pre.at[i, 1], pre_s.at[i, 1])

        def new_rows(r):
            gbuf[i, r, :] = adam(gbuf[i, r, :], pre[i, 0, r, :], pre[i, 1, r, :], wb[slot, r, :])[2]

        rows(new_rows)

        def go(a, layer, q):
            new = gbuf.at[i]
            there = whole(wo[a], a, layer, q, 2 * mine + c)
            remote(new, there, ps_s.at[mine], pr_s.at[mine], buddy).start()
            pltpu.make_async_copy(new, there, loc_s).start()

        by_array(i, go)

    def send_new(i, u):
        room(0, u)

        def go(a, layer, q):
            remote(gbuf.at[PER + i], whole(wo[a], a, layer, q, d), out_s.at[0, lax.rem(u, W)], w_s.at[z, i], dev(mine)).start()

        by_array(i, go)

    def pass_on(i, src, over):
        if over is not None:
            room(over[0], over[1])

        def go(a, layer, q):
            here = whole(wo[a], a, layer, q, 2 * src + c)
            wait(here, w_s.at[src, i])
            if over is not None:
                sems = out_s.at[over[0], lax.rem(over[1], W)], w_s.at[src, i]
                if over[0] == 0:
                    remote(here, here, *sems, dev(over[2])).start()
                else:
                    @pl.when(i < PER - X)
                    def _():
                        remote(here, here, *sems, dev(over[2])).start()

                    @pl.when(i >= PER - X)
                    def _():
                        remote(here, tail.at[jnp.maximum(i - (PER - X), 0)], *sems, dev(over[2])).start()

            remote(here, here, ps_s.at[src], pr_s.at[src], buddy).start()

        by_array(i, go)

    def pass_tail(i):
        def go(a, layer, q):
            here = tail.at[i - (PER - X)]
            wait(here, w_s.at[far, i])
            remote(here, whole(wo[a], a, layer, q, 2 * far + c), ps_s.at[far], pr_s.at[far], buddy).start()

        by_array(i, go)

    @pl.when(is_in)
    def _():
        def tick(t, carry):
            @pl.when(t < PER)
            def _():
                update(t, order(t))

            @pl.when((t >= LOCAL) & (t < LOCAL + PER))
            def _():
                pass_on(order(t - LOCAL), other, (0, t, end))

            @pl.when((t >= PER) & (t < 2 * PER))
            def _():
                pass_on(t - PER, end, (1, t, other))

            f = t - (LOCAL + PER)

            @pl.when((f >= 0) & (f < PER - X))
            def _():
                pass_on(f, far, (0, t, end))

            @pl.when(f >= PER - X)
            def _():
                pass_tail(f)

            return carry

        lax.fori_loop(0, LOCAL + 2 * PER, tick, 0)

    @pl.when(is_end)
    def _():
        def tick(t, carry):
            u = t + AHEAD

            @pl.when(u < GUEST)
            def _():
                send_sum(u)

            @pl.when(t < 6)
            def _():
                share(2 + t)

            @pl.when(t < PER)
            def _():
                update(t, t)

            @pl.when((u >= GUEST) & (u < GUEST + PER))
            def _():
                send_new(u - GUEST, u)

            @pl.when((t >= PER) & (t < PER + GUEST))
            def _():
                update_guest(t)

            got = t - LAG

            @pl.when((got >= 0) & (got < LOCAL + 2 * PER - X))
            def _():
                src = jnp.where(got < LOCAL, mine, jnp.where(got < LOCAL + PER, other, far))
                i = jnp.where(got < LOCAL, GUEST + got, jnp.where(got < LOCAL + PER, order(got - LOCAL), got - LOCAL - PER))
                pass_on(i, src, None)

            return carry

        lax.fori_loop(0, LOCAL + 2 * PER - X + LAG, tick, 0)

    for slot in range(2):
        wait(mq.at[slot], mv_s.at[slot, 0])
        wait(vq.at[slot], mv_s.at[slot, 1])
    six = gbuf.at[pl.ds(0, PER)]
    for k in range(W):
        wait(gbuf.at[0], out_s.at[0, k])

    @pl.when(is_in)
    def _():
        wait(six, loc_s)
        wait(gbuf.at[pl.ds(0, 16)], pf_s)
        for k in range(W):
            wait(gbuf.at[0], out_s.at[1, k])

    @pl.when(is_end)
    def _():
        wait(gbuf.at[pl.ds(0, PER + GUEST)], loc_s)
        wait(gbuf.at[pl.ds(0, 48)], pf_s)

    for k in range(1, 8):
        wait(nrm.at[d], ns_s.at[k])

    for k in range(4):
        less = is_end & (far == k)

        @pl.when(less)
        def _():
            part = gbuf.at[pl.ds(0, PER - X)]
            wait(part, ps_s.at[k])
            wait(part, pr_s.at[k])

        @pl.when(jnp.logical_not(less))
        def _():
            wait(six, ps_s.at[k])
            wait(six, pr_s.at[k])


def copies(*refs):
    src, dst, buf, sem_in, sem_out = refs[0:9], refs[9:18], refs[18:22], refs[22], refs[23]
    items = []
    for a in range(9):
        down, layers, rows_ = a % 3 == 2, src[a].shape[0], src[a].shape[1]
        kind = (1 if down else 0) + (0 if a < 3 else 2)
        size = buf[kind].shape[1]
        items += [(a, kind, layer, r, size) for layer in range(layers) for r in range(0, rows_, size)]
    n = len(items)
    used = [[0] * 4, []]
    slots = []
    for it in items:
        slots.append(used[0][it[1]] % COPIES)
        used[0][it[1]] += 1
    last = {}

    def start_in(k):
        a, kind, layer, r, size = items[k]
        key = (kind, slots[k])
        if key in last:
            out(last[key]).wait()
        last[key] = k
        inn(k).start()

    def inn(k):
        a, kind, layer, r, size = items[k]
        return pltpu.make_async_copy(src[a].at[layer, pl.ds(r, size)], buf[kind].at[slots[k]], sem_in.at[kind, slots[k]])

    def out(k):
        a, kind, layer, r, size = items[k]
        return pltpu.make_async_copy(buf[kind].at[slots[k]], dst[a].at[layer, pl.ds(r, size)], sem_out.at[kind, slots[k]])

    for k in range(LOOK):
        start_in(k)
    for k in range(n):
        inn(k).wait()
        out(k).start()
        if k + LOOK < n:
            start_in(k + LOOK)
    for k in last.values():
        out(k).wait()


def place(n, *refs):
    src, dst, buf, sem_in, sem_out = refs[:n], refs[n + 3 : n + 6], refs[n + 6], refs[n + 7], refs[n + 8]
    d = lax.axis_index("dp")
    z, c = d // 2, d % 2
    is_in = (z == 1) | (z == 2)
    far = jnp.where(z >= 2, 0, 3)

    def put(ref, core):
        half = X // 2
        parts = [pl.ds(0, half), pl.ds(half, X - half)]
        for h, part in enumerate(parts):
            pltpu.make_async_copy(ref.at[part], buf.at[part], sem_in.at[h]).start()
        for h, part in enumerate(parts):
            pltpu.make_async_copy(ref.at[part], buf.at[part], sem_in.at[h]).wait()
            for k in range(part.start, part.start + part.size):
                i = PER - X + k
                a = i // 8
                there = whole(dst[a], a, (i % 8) // 4, i % 4, 2 * far + core)
                pltpu.make_async_copy(buf.at[k], there, sem_out).start()
        pltpu.make_async_copy(buf, buf, sem_out).wait()

    if n == 2:
        @pl.when(is_in)
        def _():
            put(src[0], c)

    @pl.when(jnp.logical_not(is_in))
    def _():
        put(src[-1], c if n == 2 else 1 - c)


def solution(mesh):
    def step(*arrays):
        weights, m = arrays[3:6], arrays[6:9]
        count = float(8 * sum(math.prod(a.shape) for a in m))
        any_ = pl.BlockSpec(memory_space=pl.ANY)
        chunk = (CR, CC)
        dma, regular = pltpu.SemaphoreType.DMA, pltpu.SemaphoreType.REGULAR
        out = [jax.ShapeDtypeStruct(w.shape, jnp.bfloat16) for w in weights] + [jax.ShapeDtypeStruct(a.shape, jnp.float32) for a in m] * 2
        last = jax.ShapeDtypeStruct((X, *chunk), jnp.bfloat16)
        *first, tail = pl.pallas_call(
            functools.partial(kernel, count),
            out_shape=[*out, last],
            in_specs=[any_] * 12,
            out_specs=[any_] * 10,
            scratch_shapes=[
                pltpu.VMEM((2, S, *chunk), jnp.bfloat16),
                pltpu.VMEM((2, S, *chunk), jnp.bfloat16),
                pltpu.VMEM((2, U, *chunk), jnp.bfloat16),
                pltpu.VMEM((2, S, *chunk), jnp.bfloat16),
                pltpu.VMEM((LOCAL, *chunk), jnp.bfloat16),
                pltpu.VMEM((GUEST, 2, *chunk), jnp.float32),
                pltpu.VMEM((N, *chunk), jnp.bfloat16),
                pltpu.VMEM((ROWS, CC), jnp.float32),
                pltpu.VMEM((8, 8, 128), jnp.float32),
                pltpu.VMEM((1, CC), jnp.float32),
                pltpu.VMEM((2, *chunk), jnp.float32),
                pltpu.VMEM((2, *chunk), jnp.float32),
                pltpu.VMEM((2, *chunk), jnp.bfloat16),
                pltpu.VMEM((2, *chunk), jnp.float32),
                pltpu.VMEM((2, *chunk), jnp.float32),
                dma((2, S)),
                dma((2, S)),
                dma((2, S)),
                dma((2, U)),
                dma((2, S)),
                regular((2,)),
                regular((2,)),
                dma((PER,)),
                dma((LOCAL,)),
                dma((GUEST, 2)),
                dma,
                dma((4, PER)),
                dma((2, W)),
                dma((4,)),
                dma((4,)),
                dma,
                dma((2, 3)),
                dma((2, 2)),
                dma((8,)),
                dma((8,)),
            ],
            compiler_params=pltpu.CompilerParams(collective_id=0, has_side_effects=True, vmem_limit_bytes=54 * 2**20),
            cost_estimate=pl.CostEstimate(flops=10**9, bytes_accessed=3 * 10**8, transcendentals=3 * 2**20),
        )(*arrays)
        one = lax.ppermute(tail, "dp", [(2, 0), (3, 1), (4, 6), (5, 7)])
        copied = pl.pallas_call(
            copies,
            out_shape=out,
            in_specs=[any_] * 9,
            out_specs=[any_] * 9,
            scratch_shapes=[
                pltpu.VMEM((COPIES, 256, 4096), jnp.bfloat16),
                pltpu.VMEM((COPIES, 1024, 1024), jnp.bfloat16),
                pltpu.VMEM((COPIES, 128, 4096), jnp.float32),
                pltpu.VMEM((COPIES, 512, 1024), jnp.float32),
                dma((4, COPIES)),
                dma((4, COPIES)),
            ],
            compiler_params=pltpu.CompilerParams(vmem_limit_bytes=63 * 2**20),
            cost_estimate=pl.CostEstimate(flops=4 * 10**8, bytes_accessed=150 * 2**20, transcendentals=0),
        )(*first)
        one, *copied = lax.optimization_barrier((one, *copied))
        two = lax.ppermute(one, "dp", [(0, 1), (1, 0), (6, 7), (7, 6)])
        new = copied[:3]
        for held in ((tail, one), (two,)):
            n = len(held)
            new = pl.pallas_call(
                functools.partial(place, n),
                out_shape=out[:3],
                in_specs=[any_] * (n + 3),
                out_specs=[any_] * 3,
                input_output_aliases={n: 0, n + 1: 1, n + 2: 2},
                scratch_shapes=[pltpu.VMEM((X, *chunk), jnp.bfloat16), dma((2,)), dma],
                compiler_params=pltpu.CompilerParams(vmem_limit_bytes=63 * 2**20),
                cost_estimate=pl.CostEstimate(flops=10**7, bytes_accessed=4 * 2**20, transcendentals=0),
            )(*held, *new)
        return (*new, *copied[3:])

    all_of, cut = P(None, None, None), P(None, "dp", None)
    return jax.shard_map(
        step,
        mesh=mesh,
        in_specs=(P(("rep", "dp"), None, None, None),) * 3 + (all_of,) * 3 + (cut,) * 6,
        out_specs=(P("rep", None, None),) * 3 + (P("rep", "dp", None),) * 6,
        check_vma=False,
    )
```

```python
import functools
import math

import jax
import jax.numpy as jnp
from jax import lax
from jax.experimental import pallas as pl
from jax.experimental.pallas import tpu as pltpu
from jax.sharding import PartitionSpec as P

MESH = pl.DeviceIdType.MESH
CR, CC = 128, 1024
PER = 24
N = 2 * PER
S = 4
U = 8
LOCAL = 8
GUEST = PER - LOCAL
D = 2
W = 3
PAUSE = D + 1
STEPS = N + 2 * D + PAUSE
AHEAD = 2
LAG = 3
COPIES, LOOK = 6, 4
X = 8
ROWS = 16


def by_array(i, fn):
    for a in range(3):
        @pl.when((i >= 8 * a) & (i < 8 * a + 8))
        def _():
            t = i - 8 * a
            fn(a, t // 4, t % 4)


def whole(ref, a, layer, q, dd, lead=()):
    if a < 2:
        return ref.at[(*lead, layer, pl.ds(pl.multiple_of(dd * 128, 128), CR), pl.ds(pl.multiple_of(q * CC, CC), CC))]
    return ref.at[(*lead, layer, pl.ds(pl.multiple_of(dd * 512 + q * 128, 128), CR), pl.ds(0, CC))]


def kernel(count, *refs):
    terms, weights, ms, vs = refs[0:3], refs[3:6], refs[6:9], refs[9:12]
    wo, mo, vo, tail = refs[12:15], refs[15:18], refs[18:21], refs[21]
    (own, par, up, snd, ext, pre, gbuf, acc, nrm, fac, mb, vb, wb, mq, vq,
     own_s, par_s, give_s, up_s, snd_s, par_c, up_c, g_s, ext_s, pre_s, pf_s, w_s, out_s, pr_s, ps_s, loc_s, in_s, mv_s, n_s, ns_s) = refs[22:]

    d, group = lax.axis_index("dp"), lax.axis_index("rep")
    z, c = d // 2, d % 2
    right = z >= 2
    is_end = (z == 0) | (z == 3)
    is_in = (z == 1) | (z == 2)
    mine = jnp.where(right, 2, 1)
    end = jnp.where(right, 3, 0)
    other = 3 - mine
    far = 3 - end
    partner = d + 1 - 2 * c

    def dev(zz):
        return {"dp": 2 * zz + c}

    buddy = {"dp": partner}

    def chunk_of(s, n):
        late = n >= N - LOCAL
        b = jnp.where((n >= GUEST) & jnp.logical_not(late), 1, 0)
        i = jnp.where(late, n - (N - PER), n - b * GUEST)
        return (2 + b if s == 0 else 1 - b), b, i

    def block(ref, a, layer, q):
        if a < 2:
            return ref.at[layer, pl.ds(0, CR), pl.ds(pl.multiple_of(q * CC, CC), CC)]
        return ref.at[layer, pl.ds(pl.multiple_of(q * 128, 128), CR), pl.ds(0, CC)]

    def wait(ref, sem):
        pltpu.make_async_copy(ref, ref, sem).wait()

    def remote(src, dst, ssem, rsem, to):
        return pltpu.make_async_remote_copy(src, dst, ssem, rsem, device_id=to, device_id_type=MESH)

    def start_own(s, j):
        slot = lax.rem(j, S)
        home, _, i = chunk_of(s, j)
        dd = 2 * home + c

        def go(a, layer, q):
            pltpu.make_async_copy(whole(terms[a], a, layer, q, dd, (0,)), own.at[s, slot], own_s.at[s, slot]).start()

        by_array(i, go)

    def start_give(s, j):
        slot = lax.rem(j, S)
        home, _, i = chunk_of(s, j)
        dd = 2 * home + 1 - c

        def go(a, layer, q):
            remote(whole(terms[a], a, layer, q, dd, (0,)), par.at[s, slot], give_s.at[s, slot], par_s.at[s, slot], buddy).start()

        by_array(i, go)

    for s in range(2):
        for j in range(S):
            start_own(s, jnp.int32(j))

    barrier = pltpu.get_barrier_semaphore()
    for k in range(1, 8):
        pl.semaphore_signal(barrier, inc=1, device_id={"dp": lax.rem(d + k, 8)}, device_id_type=MESH)
    for k in range(1, 4):
        pl.semaphore_signal(barrier, inc=1, device_id={"rep": lax.rem(group + k, 4)}, device_id_type=MESH)
    pl.semaphore_wait(barrier, 10)

    for s in range(2):
        start_give(s, jnp.int32(0))

    acc[...] = jnp.zeros_like(acc)

    def rows(fn):
        def go(r, carry):
            fn(pl.ds(pl.multiple_of(r * ROWS, ROWS), ROWS))
            return carry

        lax.fori_loop(0, CR // ROWS, go, 0)

    def f32(x):
        return x.astype(jnp.float32)

    def process(s, k):
        zz = z if s == 0 else 3 - z
        down = z + 1 if s == 0 else z - 1
        above = z - 1 if s == 0 else z + 1
        j = k - D * zz
        pause = (zz == 2) & (j >= N - LOCAL)
        held = pause & (j < N - LOCAL + PAUSE)
        j = j - jnp.where(pause, PAUSE, 0)

        @pl.when((j >= 0) & (j < N) & jnp.logical_not(held))
        def _():
            slot, place_ = lax.rem(j, S), lax.rem(j, U)
            _, b, i = chunk_of(s, j)
            back = (zz == 3) & (j >= N - LOCAL)
            here = (zz == 2) & (j >= N - LOCAL)
            root = (zz == 3) & jnp.logical_not(back)
            on = (zz < 3) & jnp.logical_not(here)
            wait(own.at[s, slot], own_s.at[s, slot])
            wait(par.at[s, slot], par_s.at[s, slot])

            @pl.when((on & (j >= S)) | (back & (j >= N - LOCAL + S)))
            def _():
                wait(snd.at[s, slot], snd_s.at[s, slot])

            @pl.when((zz > 0) & jnp.logical_not(back))
            def _():
                wait(up.at[s, place_], up_s.at[s, place_])

            def two(r):
                return f32(own[s, slot, r, :]) + f32(par[s, slot, r, :])

            @pl.when((zz == 0) | back)
            def _():
                def add(r):
                    snd[s, slot, r, :] = two(r).astype(jnp.bfloat16)

                rows(add)

            @pl.when((zz > 0) & on)
            def _():
                def add(r):
                    snd[s, slot, r, :] = (f32(up[s, place_, r, :]) + two(r)).astype(jnp.bfloat16)

                rows(add)

            def keep(r, total):
                g = total.astype(jnp.bfloat16)
                gbuf[b * PER + i, r, :] = g
                acc[...] += f32(g) * f32(g)

            @pl.when(root)
            def _():
                rows(lambda r: keep(r, f32(up[s, place_, r, :]) + two(r)))

            @pl.when(here)
            def _():
                e = i - GUEST
                wait(ext.at[e], ext_s.at[e])
                rows(lambda r: keep(r, f32(up[s, place_, r, :]) + two(r) + f32(ext[e, r, :])))

            @pl.when(j < N - S)
            def _():
                pl.semaphore_signal(par_c.at[s], inc=1, device_id=buddy, device_id_type=MESH)

            @pl.when(((zz > 0) & (zz < 3) & (j < N - U)) | (root & (j < N - LOCAL - U)))
            def _():
                pl.semaphore_signal(up_c.at[s], inc=1, device_id=dev(above), device_id_type=MESH)

            @pl.when(j + S < N)
            def _():
                start_own(s, j + S)

            @pl.when(on)
            def _():
                @pl.when(j >= U)
                def _():
                    pl.semaphore_wait(up_c.at[s], 1)

                remote(snd.at[s, slot], up.at[s, place_], snd_s.at[s, slot], up_s.at[s, place_], dev(down)).start()

            @pl.when(back)
            def _():
                e = jnp.maximum(i - GUEST, 0)
                remote(snd.at[s, slot], ext.at[e], snd_s.at[s, slot], ext_s.at[e], dev(above)).start()

            @pl.when((j >= 1) & (j + S - 1 < N))
            def _():
                again = lax.rem(j + S - 1, S)
                pl.semaphore_wait(par_c.at[s], 1)
                wait(par.at[s, again], give_s.at[s, again])
                start_give(s, j + S - 1)

    def bring(h):
        i, kind = 4 * (h // 2) + group, lax.rem(h, 2)

        def go(a, layer, q):
            for which, ref in enumerate((ms[a], vs[a])):
                @pl.when(kind == which)
                def _():
                    remote(block(ref, a, layer, q), pre.at[i, which], pf_s, pre_s.at[i, which], dev(end)).start()

        by_array(i, go)

    def share(h):
        i, kind = 4 * (h // 2) + group, lax.rem(h, 2)
        wait(pre.at[i, kind], pre_s.at[i, kind])
        for k in range(1, 4):
            remote(pre.at[i, kind], pre.at[i, kind], pf_s, pre_s.at[i, kind], {"rep": lax.rem(group + k, 4)}).start()

    def room(link, u):
        @pl.when(u >= W)
        def _():
            wait(gbuf.at[0], out_s.at[link, lax.rem(u, W)])

    def send_sum(u):
        room(0, u)
        remote(gbuf.at[u], gbuf.at[u], out_s.at[0, lax.rem(u, W)], g_s.at[u], dev(mine)).start()

    def step(k, carry):
        @pl.when(is_in & (k < 2))
        def _():
            bring(k)

        process(0, k)
        process(1, k)

        @pl.when(k == 0)
        def _():
            for s in range(2):
                for j in range(1, S):
                    start_give(s, jnp.int32(j))

        @pl.when(is_in & (k >= N - 4) & (k < N + 2))
        def _():
            bring(k - (N - 6))

        @pl.when(is_end & ((k == 6) | (k == 7)))
        def _():
            share(k - 6)

        @pl.when(is_end & (k >= STEPS - AHEAD))
        def _():
            send_sum(k - (STEPS - AHEAD))

        return carry

    lax.fori_loop(0, STEPS, step, 0)

    def order(t):
        return jnp.where(t < LOCAL, GUEST + t, t - LOCAL)

    def start_mvw(t, i):
        slot = lax.rem(t, 2)

        def go(a, layer, q):
            pltpu.make_async_copy(block(ms[a], a, layer, q), mb.at[slot], in_s.at[slot, 0]).start()
            pltpu.make_async_copy(block(vs[a], a, layer, q), vb.at[slot], in_s.at[slot, 1]).start()
            pltpu.make_async_copy(whole(weights[a], a, layer, q, d), wb.at[slot], in_s.at[slot, 2]).start()

        by_array(i, go)

    start_mvw(jnp.int32(0), jnp.where(is_end, 0, GUEST))

    part = acc[0:8, 0:128]
    for r in range(ROWS // 8):
        for q in range(CC // 128):
            if r + q:
                part = part + acc[8 * r : 8 * r + 8, 128 * q : 128 * q + 128]
    nrm[d] = part
    for k in range(1, 8):
        remote(nrm.at[d], nrm.at[d], ns_s.at[k], n_s.at[d], {"dp": lax.rem(d + k, 8)}).start()

    for s in range(2):
        for q in range(S):
            wait(par.at[s, q], give_s.at[s, q])
        for q in range(S):
            wait(snd.at[s, q], snd_s.at[s, q])

    for k in range(8):
        @pl.when(d != k)
        def _():
            wait(nrm.at[k], n_s.at[k])

    total = ((nrm[0] + nrm[1]) + (nrm[2] + nrm[3])) + ((nrm[4] + nrm[5]) + (nrm[6] + nrm[7]))
    total = jnp.sum(total, keepdims=True)
    fac[...] = jnp.broadcast_to(jnp.minimum(1.0, 0.5 * lax.rsqrt(total / count + 1e-30)), fac.shape)

    base = jnp.where(is_end, PER, 0)

    def start_guest(t):
        slot = lax.rem(t, 2)

        def go(a, layer, q):
            pltpu.make_async_copy(whole(weights[a], a, layer, q, 2 * mine + c), wb.at[slot], in_s.at[slot, 2]).start()

        by_array(t - PER, go)

    def adam(g, m, v, w):
        g = f32(g) * fac[...]
        m = 0.9 * m + 0.1 * g
        v = 0.95 * v + 0.05 * g * g
        w = f32(w)
        return m, v, (w - 0.02 * (m * lax.rsqrt(v + 1e-8) + 0.1 * w)).astype(jnp.bfloat16)

    def update(t, i):
        slot = lax.rem(t, 2)
        at = base + i

        @pl.when(t + 1 < PER)
        def _():
            start_mvw(t + 1, jnp.where(is_end, i + 1, order(t + 1)))

        @pl.when(is_end & (t + 1 == PER))
        def _():
            start_guest(t + 1)

        wait(mb.at[slot], in_s.at[slot, 0])
        wait(vb.at[slot], in_s.at[slot, 1])
        wait(wb.at[slot], in_s.at[slot, 2])

        @pl.when(t >= 2)
        def _():
            wait(mq.at[slot], mv_s.at[slot, 0])
            wait(vq.at[slot], mv_s.at[slot, 1])

        @pl.when(is_in & (i < GUEST))
        def _():
            wait(gbuf.at[i], g_s.at[i])

        def new_rows(r):
            m, v, w = adam(gbuf[at, r, :], mb[slot, r, :], vb[slot, r, :], wb[slot, r, :])
            mq[slot, r, :] = m
            vq[slot, r, :] = v
            gbuf[at, r, :] = w

        rows(new_rows)

        @pl.when(is_in)
        def _():
            room(1, t)

        @pl.when(is_in & (t < LOCAL))
        def _():
            room(0, t)

        def go(a, layer, q):
            new = gbuf.at[at]
            there = whole(wo[a], a, layer, q, d)
            pltpu.make_async_copy(mq.at[slot], block(mo[a], a, layer, q), mv_s.at[slot, 0]).start()
            pltpu.make_async_copy(vq.at[slot], block(vo[a], a, layer, q), mv_s.at[slot, 1]).start()

            @pl.when(is_in)
            def _():
                remote(new, there, out_s.at[1, lax.rem(t, W)], w_s.at[z, i], dev(other)).start()

            @pl.when(is_in & (t < LOCAL))
            def _():
                remote(new, there, out_s.at[0, lax.rem(t, W)], w_s.at[z, i], dev(end)).start()

            remote(new, there, ps_s.at[z], pr_s.at[z], buddy).start()
            pltpu.make_async_copy(new, there, loc_s).start()

        by_array(i, go)

    def update_guest(t):
        slot = lax.rem(t, 2)
        i = t - PER

        @pl.when(t + 1 < PER + GUEST)
        def _():
            start_guest(t + 1)

        wait(wb.at[slot], in_s.at[slot, 2])

        @pl.when(lax.rem(i, 4) != group)
        def _():
            wait(pre.at[i, 0], pre_s.at[i, 0])
            wait(pre.at[i, 1], pre_s.at[i, 1])

        def new_rows(r):
            gbuf[i, r, :] = adam(gbuf[i, r, :], pre[i, 0, r, :], pre[i, 1, r, :], wb[slot, r, :])[2]

        rows(new_rows)

        def go(a, layer, q):
            new = gbuf.at[i]
            there = whole(wo[a], a, layer, q, 2 * mine + c)
            remote(new, there, ps_s.at[mine], pr_s.at[mine], buddy).start()
            pltpu.make_async_copy(new, there, loc_s).start()

        by_array(i, go)

    def send_new(i, u):
        room(0, u)

        def go(a, layer, q):
            remote(gbuf.at[PER + i], whole(wo[a], a, layer, q, d), out_s.at[0, lax.rem(u, W)], w_s.at[z, i], dev(mine)).start()

        by_array(i, go)

    def pass_on(i, src, over):
        if over is not None:
            room(over[0], over[1])

        def go(a, layer, q):
            here = whole(wo[a], a, layer, q, 2 * src + c)
            wait(here, w_s.at[src, i])
            if over is not None:
                sems = out_s.at[over[0], lax.rem(over[1], W)], w_s.at[src, i]
                if over[0] == 0:
                    remote(here, here, *sems, dev(over[2])).start()
                else:
                    @pl.when(i < PER - X)
                    def _():
                        remote(here, here, *sems, dev(over[2])).start()

                    @pl.when(i >= PER - X)
                    def _():
                        remote(here, tail.at[jnp.maximum(i - (PER - X), 0)], *sems, dev(over[2])).start()

            remote(here, here, ps_s.at[src], pr_s.at[src], buddy).start()

        by_array(i, go)

    def pass_tail(i):
        def go(a, layer, q):
            here = tail.at[i - (PER - X)]
            wait(here, w_s.at[far, i])
            remote(here, whole(wo[a], a, layer, q, 2 * far + c), ps_s.at[far], pr_s.at[far], buddy).start()

        by_array(i, go)

    @pl.when(is_in)
    def _():
        def tick(t, carry):
            @pl.when(t < PER)
            def _():
                update(t, order(t))

            @pl.when((t >= LOCAL) & (t < LOCAL + PER))
            def _():
                pass_on(order(t - LOCAL), other, (0, t, end))

            @pl.when((t >= PER) & (t < 2 * PER))
            def _():
                pass_on(t - PER, end, (1, t, other))

            f = t - (LOCAL + PER)

            @pl.when((f >= 0) & (f < PER - X))
            def _():
                pass_on(f, far, (0, t, end))

            @pl.when(f >= PER - X)
            def _():
                pass_tail(f)

            return carry

        lax.fori_loop(0, LOCAL + 2 * PER, tick, 0)

    @pl.when(is_end)
    def _():
        def tick(t, carry):
            u = t + AHEAD

            @pl.when(u < GUEST)
            def _():
                send_sum(u)

            @pl.when(t < 6)
            def _():
                share(2 + t)

            @pl.when(t < PER)
            def _():
                update(t, t)

            @pl.when((u >= GUEST) & (u < GUEST + PER))
            def _():
                send_new(u - GUEST, u)

            @pl.when((t >= PER) & (t < PER + GUEST))
            def _():
                update_guest(t)

            got = t - LAG

            @pl.when((got >= 0) & (got < LOCAL + 2 * PER - X))
            def _():
                src = jnp.where(got < LOCAL, mine, jnp.where(got < LOCAL + PER, other, far))
                i = jnp.where(got < LOCAL, GUEST + got, jnp.where(got < LOCAL + PER, order(got - LOCAL), got - LOCAL - PER))
                pass_on(i, src, None)

            return carry

        lax.fori_loop(0, LOCAL + 2 * PER - X + LAG, tick, 0)

    for slot in range(2):
        wait(mq.at[slot], mv_s.at[slot, 0])
        wait(vq.at[slot], mv_s.at[slot, 1])
    six = gbuf.at[pl.ds(0, PER)]
    for k in range(W):
        wait(gbuf.at[0], out_s.at[0, k])

    @pl.when(is_in)
    def _():
        wait(six, loc_s)
        wait(gbuf.at[pl.ds(0, 16)], pf_s)
        for k in range(W):
            wait(gbuf.at[0], out_s.at[1, k])

    @pl.when(is_end)
    def _():
        wait(gbuf.at[pl.ds(0, PER + GUEST)], loc_s)
        wait(gbuf.at[pl.ds(0, 48)], pf_s)

    for k in range(1, 8):
        wait(nrm.at[d], ns_s.at[k])

    for k in range(4):
        less = is_end & (far == k)

        @pl.when(less)
        def _():
            part = gbuf.at[pl.ds(0, PER - X)]
            wait(part, ps_s.at[k])
            wait(part, pr_s.at[k])

        @pl.when(jnp.logical_not(less))
        def _():
            wait(six, ps_s.at[k])
            wait(six, pr_s.at[k])


def copies(*refs):
    src, dst, buf, sem_in, sem_out = refs[0:9], refs[9:18], refs[18:22], refs[22], refs[23]
    items = []
    for a in range(9):
        down, layers, rows_ = a % 3 == 2, src[a].shape[0], src[a].shape[1]
        kind = (1 if down else 0) + (0 if a < 3 else 2)
        size = buf[kind].shape[1]
        items += [(a, kind, layer, r, size) for layer in range(layers) for r in range(0, rows_, size)]
    n = len(items)
    used = [[0] * 4, []]
    slots = []
    for it in items:
        slots.append(used[0][it[1]] % COPIES)
        used[0][it[1]] += 1
    last = {}

    def start_in(k):
        a, kind, layer, r, size = items[k]
        key = (kind, slots[k])
        if key in last:
            out(last[key]).wait()
        last[key] = k
        inn(k).start()

    def inn(k):
        a, kind, layer, r, size = items[k]
        return pltpu.make_async_copy(src[a].at[layer, pl.ds(r, size)], buf[kind].at[slots[k]], sem_in.at[kind, slots[k]])

    def out(k):
        a, kind, layer, r, size = items[k]
        return pltpu.make_async_copy(buf[kind].at[slots[k]], dst[a].at[layer, pl.ds(r, size)], sem_out.at[kind, slots[k]])

    for k in range(LOOK):
        start_in(k)
    for k in range(n):
        inn(k).wait()
        out(k).start()
        if k + LOOK < n:
            start_in(k + LOOK)
    for k in last.values():
        out(k).wait()


def place(n, *refs):
    src, dst, buf, sem_in, sem_out = refs[:n], refs[n + 3 : n + 6], refs[n + 6], refs[n + 7], refs[n + 8]
    d = lax.axis_index("dp")
    z, c = d // 2, d % 2
    is_in = (z == 1) | (z == 2)
    far = jnp.where(z >= 2, 0, 3)

    def put(ref, core):
        half = X // 2
        parts = [pl.ds(0, half), pl.ds(half, X - half)]
        for h, part in enumerate(parts):
            pltpu.make_async_copy(ref.at[part], buf.at[part], sem_in.at[h]).start()
        for h, part in enumerate(parts):
            pltpu.make_async_copy(ref.at[part], buf.at[part], sem_in.at[h]).wait()
            for k in range(part.start, part.start + part.size):
                i = PER - X + k
                a = i // 8
                there = whole(dst[a], a, (i % 8) // 4, i % 4, 2 * far + core)
                pltpu.make_async_copy(buf.at[k], there, sem_out).start()
        pltpu.make_async_copy(buf, buf, sem_out).wait()

    if n == 2:
        @pl.when(is_in)
        def _():
            put(src[0], c)

    @pl.when(jnp.logical_not(is_in))
    def _():
        put(src[-1], c if n == 2 else 1 - c)


def solution(mesh):
    def step(*arrays):
        weights, m = arrays[3:6], arrays[6:9]
        count = float(8 * sum(math.prod(a.shape) for a in m))
        any_ = pl.BlockSpec(memory_space=pl.ANY)
        chunk = (CR, CC)
        dma, regular = pltpu.SemaphoreType.DMA, pltpu.SemaphoreType.REGULAR
        out = [jax.ShapeDtypeStruct(w.shape, jnp.bfloat16) for w in weights] + [jax.ShapeDtypeStruct(a.shape, jnp.float32) for a in m] * 2
        last = jax.ShapeDtypeStruct((X, *chunk), jnp.bfloat16)
        *first, tail = pl.pallas_call(
            functools.partial(kernel, count),
            out_shape=[*out, last],
            in_specs=[any_] * 12,
            out_specs=[any_] * 10,
            scratch_shapes=[
                pltpu.VMEM((2, S, *chunk), jnp.bfloat16),
                pltpu.VMEM((2, S, *chunk), jnp.bfloat16),
                pltpu.VMEM((2, U, *chunk), jnp.bfloat16),
                pltpu.VMEM((2, S, *chunk), jnp.bfloat16),
                pltpu.VMEM((LOCAL, *chunk), jnp.bfloat16),
                pltpu.VMEM((GUEST, 2, *chunk), jnp.float32),
                pltpu.VMEM((N, *chunk), jnp.bfloat16),
                pltpu.VMEM((ROWS, CC), jnp.float32),
                pltpu.VMEM((8, 8, 128), jnp.float32),
                pltpu.VMEM((1, CC), jnp.float32),
                pltpu.VMEM((2, *chunk), jnp.float32),
                pltpu.VMEM((2, *chunk), jnp.float32),
                pltpu.VMEM((2, *chunk), jnp.bfloat16),
                pltpu.VMEM((2, *chunk), jnp.float32),
                pltpu.VMEM((2, *chunk), jnp.float32),
                dma((2, S)),
                dma((2, S)),
                dma((2, S)),
                dma((2, U)),
                dma((2, S)),
                regular((2,)),
                regular((2,)),
                dma((PER,)),
                dma((LOCAL,)),
                dma((GUEST, 2)),
                dma,
                dma((4, PER)),
                dma((2, W)),
                dma((4,)),
                dma((4,)),
                dma,
                dma((2, 3)),
                dma((2, 2)),
                dma((8,)),
                dma((8,)),
            ],
            compiler_params=pltpu.CompilerParams(collective_id=0, has_side_effects=True, vmem_limit_bytes=54 * 2**20),
            cost_estimate=pl.CostEstimate(flops=10**9, bytes_accessed=3 * 10**8, transcendentals=3 * 2**20),
        )(*arrays)
        one = lax.ppermute(tail, "dp", [(2, 0), (3, 1), (4, 6), (5, 7)])
        copied = pl.pallas_call(
            copies,
            out_shape=out,
            in_specs=[any_] * 9,
            out_specs=[any_] * 9,
            scratch_shapes=[
                pltpu.VMEM((COPIES, 256, 4096), jnp.bfloat16),
                pltpu.VMEM((COPIES, 1024, 1024), jnp.bfloat16),
                pltpu.VMEM((COPIES, 128, 4096), jnp.float32),
                pltpu.VMEM((COPIES, 512, 1024), jnp.float32),
                dma((4, COPIES)),
                dma((4, COPIES)),
            ],
            compiler_params=pltpu.CompilerParams(vmem_limit_bytes=63 * 2**20),
            cost_estimate=pl.CostEstimate(flops=4 * 10**8, bytes_accessed=150 * 2**20, transcendentals=0),
        )(*first)
        one, *copied = lax.optimization_barrier((one, *copied))
        two = lax.ppermute(one, "dp", [(0, 1), (1, 0), (6, 7), (7, 6)])
        new = copied[:3]
        for held in ((tail, one), (two,)):
            n = len(held)
            new = pl.pallas_call(
                functools.partial(place, n),
                out_shape=out[:3],
                in_specs=[any_] * (n + 3),
                out_specs=[any_] * 3,
                input_output_aliases={n: 0, n + 1: 1, n + 2: 2},
                scratch_shapes=[pltpu.VMEM((X, *chunk), jnp.bfloat16), dma((2,)), dma],
                compiler_params=pltpu.CompilerParams(vmem_limit_bytes=63 * 2**20),
                cost_estimate=pl.CostEstimate(flops=10**7, bytes_accessed=4 * 2**20, transcendentals=0),
            )(*held, *new)
        return (*new, *copied[3:])

    all_of, cut = P(None, None, None), P(None, "dp", None)
    return jax.shard_map(
        step,
        mesh=mesh,
        in_specs=(P(("rep", "dp"), None, None, None),) * 3 + (all_of,) * 3 + (cut,) * 6,
        out_specs=(P("rep", None, None),) * 3 + (P("rep", "dp", None),) * 6,
        check_vma=False,
    )
```
